32 devices in a mesh: dp: 4 (over y, x), fsdp: 8 (over z, core).
Axes of the slice: x: 2, y: 2, z: 4, core: 2. Of those that a mesh axis runs over, the one named last changes fastest.
Arguments:
- hidden: bfloat16 [16384, 4096], P(('dp', 'fsdp')), may hold values from -6 to 6
- queries: bfloat16 [16384, 2048], P(('dp', 'fsdp')), may hold values from -60 to 60
- cotangent: bfloat16 [16384, 2048], P(('dp', 'fsdp')), may hold values from -0.125 to 0.125
- point_start: bfloat16 [4096, 1024], P('fsdp', 'dp'), may hold values from -0.09375 to 0.09375
- point_mid: bfloat16 [4096, 1024], P('fsdp', 'dp'), may hold values from -0.09375 to 0.09375
- point_end: bfloat16 [4096, 1024], P('fsdp', 'dp'), may hold values from -0.09375 to 0.09375
- curve_time: float32 [1], replicated, may hold values from 0.15 to 0.85
Outputs:
- context: bfloat16 [16384, 2048], P(('dp', 'fsdp'))
- gradient: float32 [4096, 1024], P('fsdp', 'dp')
The draws below stay inside these ranges and needn't reach their ends.
All inputs are finite; a program needn't handle non-finite values.
Results may differ from the reference program's by a relative error of at most 0.0071.
Values may be sent and summed in bfloat16 or wider, within the bound.
A program may use at most 128 MiB of HBM per device.

```python
import math
import jax
import jax.numpy as jnp
from jax import lax

D = 4096
HQ = 16
KVH = 4
HD = 128
SEQ = 512
KVW = 512
TOKENS = 16384


def draw_queries(key, part):
    first_key = jax.random.fold_in(key, 0)
    base_draw = jnp.clip(jax.random.normal(first_key, (TOKENS, HQ * HD), jnp.float32), -4.0, 4.0)
    return base_draw.astype(jnp.bfloat16)


def spiked(drawn, own_key, source, target, blocks, factor):
    owner, partner = [(jnp.arange(drawn.shape[position]) // (drawn.shape[position] // blocks)).reshape([-1 if axis == position else 1 for axis in range(drawn.ndim)]) for position in (source, target)]
    chosen = jax.random.permutation(own_key, blocks)[partner]
    strong = (owner == chosen) | (owner == (partner + blocks // 2) % blocks)
    return jnp.where(strong, factor * drawn, drawn)


def levels(stream_key, extent, cuts, least, top_value):
    gain = 1.0
    for axis_at, parts in cuts:
        steps = jax.random.uniform(jax.random.fold_in(jax.random.fold_in(stream_key, 6), axis_at), (parts,), jnp.float32, least / len(cuts), top_value / len(cuts))
        gain = gain * jnp.repeat(jnp.exp(steps), extent[axis_at] // parts).reshape((-1,) + (1,) * (len(extent) - 1 - axis_at))
    return gain


def centred(own_key, dims, scale, limit, cuts=(), held_as=jnp.bfloat16):
    entries = scale * jax.random.normal(own_key, dims, jnp.float32)
    if cuts:
        entries = entries * levels(own_key, dims, cuts, -0.22, 0.18)
    return jnp.clip(entries, -limit, limit).astype(held_as)


def heavy_noise(own_key, extent, scale, reach, cuts, heavy, held_as=jnp.bfloat16):
    values = scale * jax.random.normal(own_key, extent, jnp.float32)
    if cuts:
        values = values * levels(own_key, extent, cuts, -0.22, 0.18)
    return jnp.clip(spiked(values, jax.random.fold_in(own_key, 3), *heavy), -reach, reach).astype(held_as)


def setup_inputs(seed: int = 0) -> dict:
    splits = jax.random.split(jax.random.key(seed), 8)
    return {
        "hidden": heavy_noise(splits[0], (TOKENS, D), 1.0, 6.0, ((0, 32),), (0, 1, 32, 2.75)),
        "queries": draw_queries(jax.random.fold_in(splits[7], 71), 0),
        "cotangent": centred(splits[2], (TOKENS, HQ * HD), (TOKENS ** -0.5), 0.125, ((0, 32),)),
        "point_start": centred(splits[3], (D, 2 * KVW), D ** -0.5, 0.09375, ((0, 8), (1, 4))),
        "point_mid": centred(splits[4], (D, 2 * KVW), D ** -0.5, 0.09375, ((0, 8), (1, 4))),
        "point_end": centred(splits[5], (D, 2 * KVW), D ** -0.5, 0.09375, ((0, 8), (1, 4))),
        "curve_time": jnp.clip(jax.random.uniform(splits[6], (1,), jnp.float32, 0.15, 0.85), 0.15, 0.85),
    }


def rope_tables(seq_len, head_dim):
    positions = jnp.arange(seq_len, dtype=jnp.float32)[:, None]
    halves_index = jnp.arange(head_dim // 2, dtype=jnp.float32)[None, :]
    inverse = jnp.exp(-(2.0 * halves_index / head_dim) * math.log(500000.0))
    angles = positions * inverse
    cosine = jnp.concatenate([jnp.cos(angles), jnp.cos(angles)], axis=1)
    sine_t = jnp.concatenate([jnp.sin(angles), jnp.sin(angles)], axis=1)
    return (cosine, sine_t)

def rotate(values_in):
    half_size = values_in.shape[-1] // 2
    return jnp.concatenate([-values_in[..., half_size:], values_in[..., :half_size]], axis=-1)

def rotate_back(values_in):
    half_size = values_in.shape[-1] // 2
    return jnp.concatenate([values_in[..., half_size:], -values_in[..., :half_size]], axis=-1)

def attend(kv_rows, query_rows, grad_rows, kv_heads, head_dim):
    seq_len = kv_rows.shape[0]
    kv_width = kv_heads * head_dim
    group_size = query_rows.shape[1] // kv_width
    width_head = group_size * head_dim
    cosine, sine_t = rope_tables(seq_len, head_dim)
    causal = jnp.arange(seq_len)[:, None] >= jnp.arange(seq_len)[None, :]
    score_scale = 1.0 / math.sqrt(head_dim)
    contexts = []
    key_grads = []
    value_grads = []
    for kv_head in range(kv_heads):
        keys_raw = kv_rows[:, kv_head * head_dim:(kv_head + 1) * head_dim].astype(jnp.float32)
        values_head = kv_rows[:, kv_width + kv_head * head_dim:kv_width + (kv_head + 1) * head_dim].astype(jnp.float32)
        keys_head = (keys_raw * cosine + rotate(keys_raw) * sine_t).astype(jnp.bfloat16).astype(jnp.float32)
        query_head = query_rows[:, kv_head * width_head:(kv_head + 1) * width_head].reshape(seq_len, group_size, head_dim).astype(jnp.float32)
        grad_head = grad_rows[:, kv_head * width_head:(kv_head + 1) * width_head].reshape(seq_len, group_size, head_dim).astype(jnp.float32)
        scores = jnp.einsum('sgd,td->gst', query_head, keys_head) * score_scale
        scores = jnp.where(causal[None], scores, -1e+30)
        top_score = lax.optimization_barrier(jnp.max(scores, axis=-1, keepdims=True))
        weights_exp = jnp.exp(scores - top_score)
        probs = weights_exp / lax.optimization_barrier(jnp.sum(weights_exp, axis=-1, keepdims=True))
        probs_low = probs.astype(jnp.bfloat16).astype(jnp.float32)
        context_head = jnp.einsum('gst,td->sgd', probs_low, values_head).astype(jnp.bfloat16)
        contexts.append(context_head.reshape(seq_len, width_head))
        prob_grad = jnp.einsum('sgd,td->gst', grad_head, values_head)
        value_grads.append(jnp.einsum('gst,sgd->td', probs_low, grad_head))
        score_grad = probs * (prob_grad - lax.optimization_barrier(jnp.sum(prob_grad * probs, axis=-1, keepdims=True))) * score_scale
        score_low = score_grad.astype(jnp.bfloat16).astype(jnp.float32)
        rot_grad = jnp.einsum('gst,sgd->td', score_low, query_head)
        key_grads.append(rot_grad * cosine + rotate_back(rot_grad * sine_t))
    context_rows = jnp.concatenate(contexts, axis=1)
    kv_grad = jnp.concatenate(key_grads + value_grads, axis=1).astype(jnp.bfloat16)
    return (context_rows, kv_grad)

def reference(hidden, queries, cotangent, point_start, point_mid, point_end, curve_time):
    t_value = curve_time[0]
    blended = ((1.0 - t_value) ** 2 * point_start.astype(jnp.float32) + 2.0 * t_value * (1.0 - t_value) * point_mid.astype(jnp.float32) + t_value ** 2 * point_end.astype(jnp.float32)).astype(jnp.bfloat16)
    kv_rows = jnp.dot(hidden, blended, preferred_element_type=jnp.float32).astype(jnp.bfloat16)
    seq_count = hidden.shape[0] // SEQ

    def one_sequence(items):
        return attend(items[0], items[1], items[2], KVH, HD)
    context_all, grad_all = lax.map(one_sequence, (kv_rows.reshape(seq_count, SEQ, -1), queries.reshape(seq_count, SEQ, -1), cotangent.reshape(seq_count, SEQ, -1)))
    context = context_all.reshape(hidden.shape[0], -1)
    kv_grad = grad_all.reshape(hidden.shape[0], -1)
    gradient = jnp.dot(hidden.T, kv_grad, preferred_element_type=jnp.float32) * (2.0 * t_value * (1.0 - t_value))
    return (context, gradient)
```

```python
import functools
import math

import jax
import jax.numpy as jnp
from jax import lax
from jax.experimental import pallas as pl
from jax.experimental.pallas import tpu as pltpu
from jax.sharding import PartitionSpec as P

KVH = 4
HD = 128
BQ = 128
MESH = pl.DeviceIdType.MESH
VMEM_LIMIT = 60 * 1024 * 1024


def rope_tables(seq_len, head_dim):
    positions = jnp.arange(seq_len, dtype=jnp.float32)[:, None]
    halves_index = jnp.arange(head_dim // 2, dtype=jnp.float32)[None, :]
    inverse = jnp.exp(-(2.0 * halves_index / head_dim) * math.log(500000.0))
    angles = positions * inverse
    cosine = jnp.concatenate([jnp.cos(angles), jnp.cos(angles)], axis=1)
    sine_t = jnp.concatenate([jnp.sin(angles), jnp.sin(angles)], axis=1)
    return (cosine, sine_t)


def rotate(x):
    half = x.shape[-1] // 2
    return jnp.concatenate([-x[..., half:], x[..., :half]], axis=-1)


def rotate_back(x):
    half = x.shape[-1] // 2
    return jnp.concatenate([x[..., half:], -x[..., :half]], axis=-1)


NN = (((1,), (0,)), ((), ()))
NT = (((1,), (1,)), ((), ()))
TN = (((0,), (0,)), ((), ()))


def mm(x, y, dims=NN):
    return lax.dot_general(x, y, dims, preferred_element_type=jnp.float32)


def attend_kernel(k_ref, v_ref, q_ref, g_ref, cos_ref, sin_ref, ctx_ref, grad_ref, kg, vg):
    seq = k_ref.shape[0]
    group = q_ref.shape[1] // HD
    scale = 1.0 / math.sqrt(HD)
    to_base2 = scale * math.log2(math.e)
    raw = k_ref[...].astype(jnp.float32)
    cosine, sine_t = cos_ref[...], sin_ref[...]
    keys = (raw * cosine + rotate(raw) * sine_t).astype(jnp.bfloat16)
    values = v_ref[...]
    values_t = values.astype(jnp.float32).T.astype(jnp.bfloat16)
    kg[...] = jnp.zeros_like(kg)
    vg[...] = jnp.zeros_like(vg)
    for start in range(0, seq, BQ):
        nk = start + BQ
        rows = slice(start, nk)
        qs = jnp.concatenate([q_ref[rows, g * HD:(g + 1) * HD] for g in range(group)], axis=0)
        gs = jnp.concatenate([g_ref[rows, g * HD:(g + 1) * HD] for g in range(group)], axis=0)
        s = mm(keys[:nk], qs, NT)
        key_at = lax.broadcasted_iota(jnp.int32, (BQ, group * BQ), 0)
        query_at = lax.broadcasted_iota(jnp.int32, (BQ, group * BQ), 1) % BQ
        last = jnp.where(key_at <= query_at, s[start:], -1e30)
        s = last if start == 0 else jnp.concatenate([s[:start], last], axis=0)
        top = jnp.max(s, axis=0, keepdims=True)
        w = jnp.exp2((s - top) * to_base2)
        p = w * (1.0 / jnp.sum(w, axis=0, keepdims=True))
        p_low = p.astype(jnp.bfloat16)
        ctx_t = mm(values_t[:, :nk], p_low)
        dp = mm(values[:nk], gs, NT)
        vg[:nk] += mm(p_low, gs)
        delta = jnp.sum(dp * p, axis=0, keepdims=True)
        ds = (p * ((dp - delta) * scale)).astype(jnp.bfloat16)
        kg[:nk] += mm(ds, qs)
        ctx = ctx_t.T.astype(jnp.bfloat16)
        for g in range(group):
            ctx_ref[rows, g * HD:(g + 1) * HD] = ctx[g * BQ:(g + 1) * BQ]
    rot = kg[...]
    grad_ref[0] = (rot * cosine + rotate_back(rot * sine_t)).astype(jnp.bfloat16)
    grad_ref[1] = vg[...].astype(jnp.bfloat16)


def attend(kv_rows, queries, cotangent):
    seq = kv_rows.shape[0]
    heads = kv_rows.shape[1] // (2 * HD)
    width = queries.shape[1] // heads
    cosine, sine_t = rope_tables(seq, HD)
    return pl.pallas_call(
        attend_kernel,
        grid=(heads,),
        out_shape=(
            jax.ShapeDtypeStruct(queries.shape, jnp.bfloat16),
            jax.ShapeDtypeStruct((2, seq, heads * HD), jnp.bfloat16),
        ),
        in_specs=[
            pl.BlockSpec((seq, HD), lambda j: (0, j)),
            pl.BlockSpec((seq, HD), lambda j: (0, j + heads)),
            pl.BlockSpec((seq, width), lambda j: (0, j)),
            pl.BlockSpec((seq, width), lambda j: (0, j)),
            pl.BlockSpec((seq, HD), lambda j: (0, 0)),
            pl.BlockSpec((seq, HD), lambda j: (0, 0)),
        ],
        out_specs=(
            pl.BlockSpec((seq, width), lambda j: (0, j)),
            pl.BlockSpec((2, seq, HD), lambda j: (0, 0, j)),
        ),
        scratch_shapes=[pltpu.VMEM((seq, HD), jnp.float32), pltpu.VMEM((seq, HD), jnp.float32)],
        compiler_params=pltpu.CompilerParams(vmem_limit_bytes=VMEM_LIMIT),
        name="attend",
    )(kv_rows, kv_rows, queries, cotangent, cosine, sine_t)


def place(dims):
    dp, fs = lax.axis_index("dp"), lax.axis_index("fsdp")
    return (dp // dims[1], dp % dims[1], fs // 2), fs % 2


def target(dims, at, core, axis=None, offset=0):
    at = list(at)
    if axis is not None:
        at[axis] = (at[axis] + offset) % dims[axis]
    return (at[0] * dims[1] + at[1], at[2] * 2 + core)


def greet(peers):
    barrier = pltpu.get_barrier_semaphore()
    for peer in peers:
        pl.semaphore_signal(barrier, inc=1, device_id=peer, device_id_type=MESH)
    pl.semaphore_wait(barrier, len(peers))


def send(src, dst, send_sem, recv_sem, peer):
    return pltpu.make_async_remote_copy(
        src_ref=src, dst_ref=dst, send_sem=send_sem, recv_sem=recv_sem,
        device_id=peer, device_id_type=MESH)


ORDER = ((1, 0), (0, 1))


def reduce_kernel(dims, x1_ref, x2_ref, y1_ref, y2_ref, out_ref, *scratch):
    halves = [scratch[:11], scratch[11:]]
    at, core = place(dims)
    depth = dims[2]
    rows, cols = out_ref.shape
    half = rows // 2
    parts = y1_ref.shape[0]
    width = y1_ref.shape[2]
    peers = [target(dims, at, core, axis, k) for axis in range(3) for k in range(1, dims[axis])]
    greet(peers)

    def first_copy(h, k1, zz):
        d1 = ORDER[h][0]
        part, r1, s1, q1 = halves[h][0], halves[h][1], halves[h][5], halves[h][6]
        v1 = (at[d1] + k1) % dims[d1]
        return send(part.at[zz, v1], r1.at[k1 - 1, zz], s1.at[k1 - 1, zz], q1.at[k1 - 1, zz],
                    target(dims, at, core, d1, k1))

    def second_copy(h, k2, zz):
        d2 = ORDER[h][1]
        sum2, r2, s2, q2 = halves[h][2], halves[h][3], halves[h][7], halves[h][8]
        return send(sum2.at[k2 - 1, zz], r2.at[k2 - 1, zz], s2.at[k2 - 1, zz], q2.at[k2 - 1, zz],
                    target(dims, at, core, d2, k2))

    def third_copy(h, k):
        r3, s3, q3 = halves[h][4], halves[h][9], halves[h][10]
        part = halves[h][0]
        zz = (at[2] + k) % depth
        d1, d2 = ORDER[h]
        return send(part.at[zz, at[d1], at[d2]], r3.at[k - 1], s3.at[k - 1], q3.at[k - 1],
                    target(dims, at, core, 2, k))

    @pl.loop(1, depth + 1)
    def _(step):
        zz = (at[2] + step) % depth
        first = pl.multiple_of(zz * rows, rows)
        x1 = x1_ref[:, pl.ds(first, rows)]
        x2 = x2_ref[:, pl.ds(first, rows)]
        for part in range(parts):
            r = (mm(x1, y1_ref[part], TN) + mm(x2, y2_ref[part], TN)).astype(jnp.bfloat16)
            for i in range(width // cols):
                dp = part * (width // cols) + i
                where = (dp // dims[1], dp % dims[1])
                for h in range(2):
                    d1, d2 = ORDER[h]
                    halves[h][0][zz, where[d1], where[d2]] = (
                        r[h * half:(h + 1) * half, i * cols:(i + 1) * cols])
        for h in range(2):
            for k1 in range(1, dims[ORDER[h][0]]):
                first_copy(h, k1, zz).start()

    def keep1(h, zz, v2):
        d1, d2 = ORDER[h]
        part, r1 = halves[h][0], halves[h][1]
        total = part[zz, at[d1], v2].astype(jnp.float32)
        for k1 in range(1, dims[d1]):
            total += r1[k1 - 1, zz, v2].astype(jnp.float32)
        return total

    def second(step):
        zz = (at[2] + step) % depth
        for h in range(2):
            d1, d2 = ORDER[h]
            for k1 in range(1, dims[d1]):
                first_copy(h, k1, zz).wait_recv()
            for k2 in range(1, dims[d2]):
                v2 = (at[d2] + k2) % dims[d2]
                halves[h][2][k2 - 1, zz] = keep1(h, zz, v2).astype(jnp.bfloat16)
                second_copy(h, k2, zz).start()

    def keep2(h, zz):
        d1, d2 = ORDER[h]
        total = keep1(h, zz, at[d2])
        for k2 in range(1, dims[d2]):
            second_copy(h, k2, zz).wait_recv()
        for k2 in range(1, dims[d2]):
            total += halves[h][3][k2 - 1, zz].astype(jnp.float32)
        return total

    def third(step):
        zz = (at[2] + step) % depth
        for h in range(2):
            d1, d2 = ORDER[h]
            halves[h][0][zz, at[d1], at[d2]] = keep2(h, zz).astype(jnp.bfloat16)
            third_copy(h, step).start()

    second(1)

    @pl.loop(2, depth + 1)
    def _(step):
        second(step)
        third(step - 1)

    for h in range(2):
        total = keep2(h, at[2])
        for k in range(1, depth):
            third_copy(h, k).wait_recv()
            total += halves[h][4][k - 1].astype(jnp.float32)
        out_ref[h * half:(h + 1) * half] = total

    @pl.loop(0, depth)
    def _(zz):
        for h in range(2):
            for k1 in range(1, dims[ORDER[h][0]]):
                first_copy(h, k1, zz).wait_send()
            for k2 in range(1, dims[ORDER[h][1]]):
                second_copy(h, k2, zz).wait_send()

    @pl.loop(1, depth)
    def _(k):
        for h in range(2):
            third_copy(h, k).wait_send()


def reduce_gradient(dims, x1, x2, y1, y2, rows, cols):
    half = rows // 2
    scratch = []
    for h in range(2):
        n1, n2 = dims[ORDER[h][0]], dims[ORDER[h][1]]
        z = dims[2]
        scratch += [
            pltpu.VMEM((z, n1, n2, half, cols), jnp.bfloat16),
            pltpu.VMEM((n1 - 1, z, n2, half, cols), jnp.bfloat16),
            pltpu.VMEM((n2 - 1, z, half, cols), jnp.bfloat16),
            pltpu.VMEM((n2 - 1, z, half, cols), jnp.bfloat16),
            pltpu.VMEM((z - 1, half, cols), jnp.bfloat16),
            pltpu.SemaphoreType.DMA((n1 - 1, z)), pltpu.SemaphoreType.DMA((n1 - 1, z)),
            pltpu.SemaphoreType.DMA((n2 - 1, z)), pltpu.SemaphoreType.DMA((n2 - 1, z)),
            pltpu.SemaphoreType.DMA((z - 1,)), pltpu.SemaphoreType.DMA((z - 1,)),
        ]
    vmem = pl.BlockSpec(memory_space=pltpu.VMEM)
    return pl.pallas_call(
        functools.partial(reduce_kernel, dims),
        out_shape=jax.ShapeDtypeStruct((rows, cols), jnp.float32),
        in_specs=[vmem] * 4,
        out_specs=vmem,
        scratch_shapes=scratch,
        compiler_params=pltpu.CompilerParams(
            collective_id=1, has_side_effects=True, vmem_limit_bytes=VMEM_LIMIT),
        name="reduce_gradient",
    )(x1, x2, y1, y2)


def local(dims, hidden, queries, cotangent, point_start, point_mid, point_end, curve_time):
    t_value = curve_time[0]
    blended = (
        (1.0 - t_value) ** 2 * point_start.astype(jnp.float32)
        + 2.0 * t_value * (1.0 - t_value) * point_mid.astype(jnp.float32)
        + t_value**2 * point_end.astype(jnp.float32)
    ).astype(jnp.bfloat16)
    seq_len, model_width = hidden.shape
    rows, cols = point_mid.shape
    core = lax.axis_index("fsdp") % 2
    swap = [(i, i ^ 1) for i in range(2 * dims[2])]
    split = hidden.reshape(seq_len, dims[2], 2, rows)
    own_first = core == 0
    mine = jnp.where(own_first, split[:, :, 0], split[:, :, 1]).reshape(seq_len, -1)
    others = jnp.where(own_first, split[:, :, 1], split[:, :, 0]).reshape(seq_len, -1)
    x2 = lax.ppermute(others, "fsdp", swap)

    columns_full = lax.all_gather(blended, "dp", axis=1, tiled=True)
    full = lax.all_gather(columns_full, "fsdp", axis=0, tiled=True)
    kv_rows = jnp.dot(hidden, full, preferred_element_type=jnp.float32).astype(jnp.bfloat16)

    context, kv_grad = attend(kv_rows, queries, cotangent)
    kv_other = lax.ppermute(kv_grad, "fsdp", swap)
    gradient = reduce_gradient(dims, mine, x2, kv_grad, kv_other, rows, cols)
    return (context, gradient * (2.0 * t_value * (1.0 - t_value)))


def solution(mesh):
    dp, fsdp = mesh.shape["dp"], mesh.shape["fsdp"]
    dims = (dp // 2, 2, fsdp // 2)
    return jax.shard_map(
        functools.partial(local, dims),
        mesh=mesh,
        in_specs=(
            P(("dp", "fsdp"), None),
            P(("dp", "fsdp"), None),
            P(("dp", "fsdp"), None),
            P("fsdp", "dp"),
            P("fsdp", "dp"),
            P("fsdp", "dp"),
            P(),
        ),
        out_specs=(P(("dp", "fsdp"), None), P("fsdp", "dp")),
        check_vma=False,
    )
```

```python
import functools
import math

import jax
import jax.numpy as jnp
from jax import lax
from jax.experimental import pallas as pl
from jax.experimental.pallas import tpu as pltpu
from jax.sharding import PartitionSpec as P

KVH = 4
HD = 128
BQ = 128
MESH = pl.DeviceIdType.MESH
VMEM_LIMIT = 60 * 1024 * 1024


def rope_tables(seq_len, head_dim):
    positions = jnp.arange(seq_len, dtype=jnp.float32)[:, None]
    halves_index = jnp.arange(head_dim // 2, dtype=jnp.float32)[None, :]
    inverse = jnp.exp(-(2.0 * halves_index / head_dim) * math.log(500000.0))
    angles = positions * inverse
    cosine = jnp.concatenate([jnp.cos(angles), jnp.cos(angles)], axis=1)
    sine_t = jnp.concatenate([jnp.sin(angles), jnp.sin(angles)], axis=1)
    return (cosine, sine_t)


def rotate(x):
    half = x.shape[-1] // 2
    return jnp.concatenate([-x[..., half:], x[..., :half]], axis=-1)


def rotate_back(x):
    half = x.shape[-1] // 2
    return jnp.concatenate([x[..., half:], -x[..., :half]], axis=-1)


NN = (((1,), (0,)), ((), ()))
NT = (((1,), (1,)), ((), ()))
TN = (((0,), (0,)), ((), ()))


def mm(x, y, dims=NN):
    return lax.dot_general(x, y, dims, preferred_element_type=jnp.float32)


def attend_kernel(k_ref, v_ref, q_ref, g_ref, cos_ref, sin_ref, ctx_ref, grad_ref, kg, vg):
    seq = k_ref.shape[0]
    group = q_ref.shape[1] // HD
    scale = 1.0 / math.sqrt(HD)
    to_base2 = scale * math.log2(math.e)
    raw = k_ref[...].astype(jnp.float32)
    cosine, sine_t = cos_ref[...], sin_ref[...]
    keys = (raw * cosine + rotate(raw) * sine_t).astype(jnp.bfloat16)
    values = v_ref[...]
    values_t = values.astype(jnp.float32).T.astype(jnp.bfloat16)
    kg[...] = jnp.zeros_like(kg)
    vg[...] = jnp.zeros_like(vg)
    for start in range(0, seq, BQ):
        nk = start + BQ
        rows = slice(start, nk)
        qs = jnp.concatenate([q_ref[rows, g * HD:(g + 1) * HD] for g in range(group)], axis=0)
        gs = jnp.concatenate([g_ref[rows, g * HD:(g + 1) * HD] for g in range(group)], axis=0)
        s = mm(keys[:nk], qs, NT)
        key_at = lax.broadcasted_iota(jnp.int32, (BQ, group * BQ), 0)
        query_at = lax.broadcasted_iota(jnp.int32, (BQ, group * BQ), 1) % BQ
        last = jnp.where(key_at <= query_at, s[start:], -1e30)
        s = last if start == 0 else jnp.concatenate([s[:start], last], axis=0)
        top = jnp.max(s, axis=0, keepdims=True)
        w = jnp.exp2((s - top) * to_base2)
        p = w * (1.0 / jnp.sum(w, axis=0, keepdims=True))
        p_low = p.astype(jnp.bfloat16)
        ctx_t = mm(values_t[:, :nk], p_low)
        dp = mm(values[:nk], gs, NT)
        vg[:nk] += mm(p_low, gs)
        delta = jnp.sum(dp * p, axis=0, keepdims=True)
        ds = (p * ((dp - delta) * scale)).astype(jnp.bfloat16)
        kg[:nk] += mm(ds, qs)
        ctx = ctx_t.T.astype(jnp.bfloat16)
        for g in range(group):
            ctx_ref[rows, g * HD:(g + 1) * HD] = ctx[g * BQ:(g + 1) * BQ]
    rot = kg[...]
    grad_ref[0] = (rot * cosine + rotate_back(rot * sine_t)).astype(jnp.bfloat16)
    grad_ref[1] = vg[...].astype(jnp.bfloat16)


def attend(kv_rows, queries, cotangent):
    seq = kv_rows.shape[0]
    heads = kv_rows.shape[1] // (2 * HD)
    width = queries.shape[1] // heads
    cosine, sine_t = rope_tables(seq, HD)
    return pl.pallas_call(
        attend_kernel,
        grid=(heads,),
        out_shape=(
            jax.ShapeDtypeStruct(queries.shape, jnp.bfloat16),
            jax.ShapeDtypeStruct((2, seq, heads * HD), jnp.bfloat16),
        ),
        in_specs=[
            pl.BlockSpec((seq, HD), lambda j: (0, j)),
            pl.BlockSpec((seq, HD), lambda j: (0, j + heads)),
            pl.BlockSpec((seq, width), lambda j: (0, j)),
            pl.BlockSpec((seq, width), lambda j: (0, j)),
            pl.BlockSpec((seq, HD), lambda j: (0, 0)),
            pl.BlockSpec((seq, HD), lambda j: (0, 0)),
        ],
        out_specs=(
            pl.BlockSpec((seq, width), lambda j: (0, j)),
            pl.BlockSpec((2, seq, HD), lambda j: (0, 0, j)),
        ),
        scratch_shapes=[pltpu.VMEM((seq, HD), jnp.float32), pltpu.VMEM((seq, HD), jnp.float32)],
        compiler_params=pltpu.CompilerParams(vmem_limit_bytes=VMEM_LIMIT),
        name="attend",
    )(kv_rows, kv_rows, queries, cotangent, cosine, sine_t)


ORDER = ((1, 0), (0, 1))


def place(dims):
    dp, fs = lax.axis_index("dp"), lax.axis_index("fsdp")
    return (dp // dims[1], dp % dims[1], fs // 2), fs % 2


def target(dims, at, core, axis=None, offset=0):
    at = list(at)
    if axis is not None:
        at[axis] = (at[axis] + offset) % dims[axis]
    return (at[0] * dims[1] + at[1], at[2] * 2 + core)


def greet(peers):
    barrier = pltpu.get_barrier_semaphore()
    for peer in peers:
        pl.semaphore_signal(barrier, inc=1, device_id=peer, device_id_type=MESH)
    pl.semaphore_wait(barrier, len(peers))


def send(src, dst, send_sem, recv_sem, peer):
    return pltpu.make_async_remote_copy(
        src_ref=src, dst_ref=dst, send_sem=send_sem, recv_sem=recv_sem,
        device_id=peer, device_id_type=MESH)


def all_peers(dims, at, core):
    peers = [target(dims, at, core, axis, k) for axis in range(3) for k in range(1, dims[axis])]
    return peers + [target(dims, at, 1 - core)]


def gather_kernel(dims, block_ref, hidden_ref, kv_ref, x2_ref, full, acc, load_sem, x_send, x_recv,
                  recv, z_send, s2, s3, c_send):
    at, core = place(dims)
    depth = dims[2]
    rows, cols = block_ref.shape
    half = rows // 2
    other = target(dims, at, 1 - core)

    def piece(c, h, zz, pos):
        return full.at[c, zz, pos[0], pos[1], pl.ds(h * half, half)]

    def cell(h, zz, pos):
        return recv.at[core, h, zz, pos[0], pos[1]]

    def moved(axis, k):
        pos = [at[0], at[1]]
        pos[axis] = (pos[axis] + k) % dims[axis]
        return pos

    def push(h, zz, pos, send_sem, peer):
        ref = piece(core, h, zz, pos)
        return send(ref, ref, send_sem, cell(h, zz, pos), peer)

    def to_z(h, k):
        return push(h, at[2], at[:2], z_send.at[h, k - 1], target(dims, at, core, 2, k))

    def to_second(h, zz, k):
        d2 = ORDER[1 - h][0]
        return push(h, zz, at[:2], s2[h].at[k - 1, zz], target(dims, at, core, d2, k))

    def to_third(h, zz, pos, k):
        d2, d3 = ORDER[1 - h]
        return push(h, zz, pos, s3[h].at[k - 1, zz, pos[d2]], target(dims, at, core, d3, k))

    def to_core(h, zz, pos):
        ref = piece(core, h, zz, pos)
        return send(ref, ref, c_send.at[h, zz, pos[0], pos[1]], cell(h, zz, pos), other)

    def swap(zz):
        src = pl.multiple_of((2 * zz + 1 - core) * rows, rows)
        dst = pl.multiple_of(zz * rows, rows)
        return send(hidden_ref.at[:, pl.ds(src, rows)], x2_ref.at[:, pl.ds(dst, rows)],
                    x_send.at[zz], x_recv.at[zz], other)

    def arrived(c, h, zz, pos):
        ref = piece(c, h, zz, pos)
        send(ref, ref, c_send.at[h, zz, pos[0], pos[1]], recv.at[c, h, zz, pos[0], pos[1]],
             other).wait_recv()

    def relay_first(h, zz):
        d2, d3 = ORDER[1 - h]
        for k in range(1, dims[d2]):
            to_second(h, zz, k).start()
        for k in range(1, dims[d3]):
            to_third(h, zz, at[:2], k).start()
        to_core(h, zz, at[:2]).start()

    def relay_second(zz):
        for h in range(2):
            d2, d3 = ORDER[1 - h]
            for k2 in range(1, dims[d2]):
                pos = moved(d2, k2)
                arrived(core, h, zz, pos)
                for k in range(1, dims[d3]):
                    to_third(h, zz, pos, k).start()
                to_core(h, zz, pos).start()

    def product(c, zz, first):
        x = hidden_ref[:, pl.ds(pl.multiple_of((2 * zz + c) * rows, rows), rows)]
        for dp in range(dims[0] * dims[1]):
            w = full[c, zz, dp // dims[1], dp % dims[1]]
            got = mm(x, w)
            if first:
                acc[:, dp * cols:(dp + 1) * cols] = got
            else:
                acc[:, dp * cols:(dp + 1) * cols] += got

    def relay_third(zz):
        for h in range(2):
            d2, d3 = ORDER[1 - h]
            for k3 in range(1, dims[d3]):
                for k2 in range(dims[d2]):
                    pos = moved(d3, k3)
                    pos[d2] = (at[d2] + k2) % dims[d2]
                    arrived(core, h, zz, pos)
                    to_core(h, zz, pos).start()

    def from_core(zz):
        for h in range(2):
            for i in range(dims[0]):
                for j in range(dims[1]):
                    arrived(1 - core, h, zz, (i, j))

    loads = [pltpu.make_async_copy(block_ref.at[pl.ds(h * half, half)], piece(core, h, at[2], at[:2]),
                                   load_sem.at[h]) for h in range(2)]
    for load in loads:
        load.start()
    greet(all_peers(dims, at, core))
    for load in loads:
        load.wait()
    for h in range(2):
        for k in range(1, depth):
            to_z(h, k).start()
        relay_first(h, at[2])

    @pl.loop(1, depth)
    def _(k):
        zz = (at[2] + depth - k) % depth
        for h in range(2):
            arrived(core, h, zz, at[:2])
            relay_first(h, zz)
        relay_second((zz + 1) % depth)

    relay_second((at[2] + 1) % depth)

    @pl.loop(0, depth)
    def _(zz):
        swap(zz).start()

    relay_third(at[2])
    product(core, at[2], True)

    @pl.loop(1, depth)
    def _(k):
        zz = (at[2] + depth - k) % depth
        before = (zz + 1) % depth
        relay_third(zz)
        product(core, zz, False)
        from_core(before)
        product(1 - core, before, False)

    last = (at[2] + 1) % depth
    from_core(last)
    product(1 - core, last, False)
    kv_ref[...] = acc[...].astype(jnp.bfloat16)

    for h in range(2):
        for k in range(1, depth):
            to_z(h, k).wait_send()

    @pl.loop(0, depth)
    def _(zz):
        swap(zz).wait()
        for h in range(2):
            d2, d3 = ORDER[1 - h]
            for k in range(1, dims[d2]):
                to_second(h, zz, k).wait_send()
            for k in range(1, dims[d3]):
                for k2 in range(dims[d2]):
                    pos = moved(d2, k2)
                    to_third(h, zz, pos, k).wait_send()
            for i in range(dims[0]):
                for j in range(dims[1]):
                    to_core(h, zz, (i, j)).wait_send()


def gather_project(dims, blended, hidden):
    rows, cols = blended.shape
    seq = hidden.shape[0]
    a, b, z = dims
    width = a * b * cols
    sem = pltpu.SemaphoreType.DMA

    def body(*refs):
        gather_kernel(dims, *refs[:10], refs[10], (refs[11], refs[12]), (refs[13], refs[14]), refs[15])

    def sems(h):
        d2, d3 = ORDER[1 - h]
        return dims[d2], dims[d3]

    vmem = pl.BlockSpec(memory_space=pltpu.VMEM)
    return pl.pallas_call(
        body,
        out_shape=(
            jax.ShapeDtypeStruct((seq, width), jnp.bfloat16),
            jax.ShapeDtypeStruct((seq, z * rows), jnp.bfloat16),
        ),
        in_specs=[pl.BlockSpec(memory_space=pl.ANY), vmem],
        out_specs=(vmem, pl.BlockSpec(memory_space=pl.ANY)),
        scratch_shapes=[
            pltpu.VMEM((2, z, a, b, rows, cols), jnp.bfloat16),
            pltpu.VMEM((seq, width), jnp.float32),
            sem((2,)), sem((z,)), sem((z,)),
            sem((2, 2, z, a, b)),
            sem((2, z - 1)),
            *[sem((sems(h)[0] - 1, z)) for h in range(2)],
            *[sem((sems(h)[1] - 1, z, sems(h)[0])) for h in range(2)],
            sem((2, z, a, b)),
        ],
        compiler_params=pltpu.CompilerParams(
            collective_id=2, has_side_effects=True, vmem_limit_bytes=VMEM_LIMIT),
        name="gather_project",
    )(blended, hidden)


def reduce_kernel(dims, x1_ref, x2_ref, y1_ref, out_ref, y2_ref, swap_send, swap_recv, *scratch):
    halves = [scratch[:11], scratch[11:]]
    at, core = place(dims)
    depth = dims[2]
    rows, cols = out_ref.shape
    half = rows // 2
    parts = y1_ref.shape[0]
    width = y1_ref.shape[2]
    other = target(dims, at, 1 - core)
    greet(all_peers(dims, at, core))
    swap = send(y1_ref, y2_ref, swap_send, swap_recv, other)
    swap.start()
    swap.wait()

    def first_copy(h, k1, zz):
        d1 = ORDER[h][0]
        part, r1, s1, q1 = halves[h][0], halves[h][1], halves[h][5], halves[h][6]
        v1 = (at[d1] + k1) % dims[d1]
        return send(part.at[zz, v1], r1.at[k1 - 1, zz], s1.at[k1 - 1, zz], q1.at[k1 - 1, zz],
                    target(dims, at, core, d1, k1))

    def second_copy(h, k2, zz):
        d2 = ORDER[h][1]
        sum2, r2, s2, q2 = halves[h][2], halves[h][3], halves[h][7], halves[h][8]
        return send(sum2.at[k2 - 1, zz], r2.at[k2 - 1, zz], s2.at[k2 - 1, zz], q2.at[k2 - 1, zz],
                    target(dims, at, core, d2, k2))

    def third_copy(h, k):
        r3, s3, q3 = halves[h][4], halves[h][9], halves[h][10]
        part = halves[h][0]
        zz = (at[2] + k) % depth
        d1, d2 = ORDER[h]
        return send(part.at[zz, at[d1], at[d2]], r3.at[k - 1], s3.at[k - 1], q3.at[k - 1],
                    target(dims, at, core, 2, k))

    @pl.loop(1, depth + 1)
    def _(step):
        zz = (at[2] + step) % depth
        x1 = x1_ref[:, pl.ds(pl.multiple_of((2 * zz + core) * rows, rows), rows)]
        x2 = x2_ref[:, pl.ds(pl.multiple_of(zz * rows, rows), rows)]
        for part in range(parts):
            r = (mm(x1, y1_ref[part], TN) + mm(x2, y2_ref[part], TN)).astype(jnp.bfloat16)
            for i in range(width // cols):
                dp = part * (width // cols) + i
                where = (dp // dims[1], dp % dims[1])
                for h in range(2):
                    d1, d2 = ORDER[h]
                    halves[h][0][zz, where[d1], where[d2]] = (
                        r[h * half:(h + 1) * half, i * cols:(i + 1) * cols])
        for h in range(2):
            for k1 in range(1, dims[ORDER[h][0]]):
                first_copy(h, k1, zz).start()

    def keep1(h, zz, v2):
        d1, d2 = ORDER[h]
        part, r1 = halves[h][0], halves[h][1]
        total = part[zz, at[d1], v2].astype(jnp.float32)
        for k1 in range(1, dims[d1]):
            total += r1[k1 - 1, zz, v2].astype(jnp.float32)
        return total

    def second(step):
        zz = (at[2] + step) % depth
        for h in range(2):
            d1, d2 = ORDER[h]
            for k1 in range(1, dims[d1]):
                first_copy(h, k1, zz).wait_recv()
            for k2 in range(1, dims[d2]):
                v2 = (at[d2] + k2) % dims[d2]
                halves[h][2][k2 - 1, zz] = keep1(h, zz, v2).astype(jnp.bfloat16)
                second_copy(h, k2, zz).start()

    def keep2(h, zz):
        d1, d2 = ORDER[h]
        total = keep1(h, zz, at[d2])
        for k2 in range(1, dims[d2]):
            second_copy(h, k2, zz).wait_recv()
        for k2 in range(1, dims[d2]):
            total += halves[h][3][k2 - 1, zz].astype(jnp.float32)
        return total

    def third(step):
        zz = (at[2] + step) % depth
        for h in range(2):
            d1, d2 = ORDER[h]
            halves[h][0][zz, at[d1], at[d2]] = keep2(h, zz).astype(jnp.bfloat16)
            third_copy(h, step).start()

    second(1)

    @pl.loop(2, depth + 1)
    def _(step):
        second(step)
        third(step - 1)

    for h in range(2):
        total = keep2(h, at[2])
        for k in range(1, depth):
            third_copy(h, k).wait_recv()
            total += halves[h][4][k - 1].astype(jnp.float32)
        out_ref[h * half:(h + 1) * half] = total

    @pl.loop(0, depth)
    def _(zz):
        for h in range(2):
            for k1 in range(1, dims[ORDER[h][0]]):
                first_copy(h, k1, zz).wait_send()
            for k2 in range(1, dims[ORDER[h][1]]):
                second_copy(h, k2, zz).wait_send()

    @pl.loop(1, depth)
    def _(k):
        for h in range(2):
            third_copy(h, k).wait_send()


def reduce_gradient(dims, x1, x2, y1, rows, cols):
    half = rows // 2
    scratch = [pltpu.VMEM(y1.shape, y1.dtype), pltpu.SemaphoreType.DMA, pltpu.SemaphoreType.DMA]
    for h in range(2):
        n1, n2 = dims[ORDER[h][0]], dims[ORDER[h][1]]
        z = dims[2]
        scratch += [
            pltpu.VMEM((z, n1, n2, half, cols), jnp.bfloat16),
            pltpu.VMEM((n1 - 1, z, n2, half, cols), jnp.bfloat16),
            pltpu.VMEM((n2 - 1, z, half, cols), jnp.bfloat16),
            pltpu.VMEM((n2 - 1, z, half, cols), jnp.bfloat16),
            pltpu.VMEM((z - 1, half, cols), jnp.bfloat16),
            pltpu.SemaphoreType.DMA((n1 - 1, z)), pltpu.SemaphoreType.DMA((n1 - 1, z)),
            pltpu.SemaphoreType.DMA((n2 - 1, z)), pltpu.SemaphoreType.DMA((n2 - 1, z)),
            pltpu.SemaphoreType.DMA((z - 1,)), pltpu.SemaphoreType.DMA((z - 1,)),
        ]
    vmem = pl.BlockSpec(memory_space=pltpu.VMEM)
    return pl.pallas_call(
        functools.partial(reduce_kernel, dims),
        out_shape=jax.ShapeDtypeStruct((rows, cols), jnp.float32),
        in_specs=[vmem] * 3,
        out_specs=vmem,
        scratch_shapes=scratch,
        compiler_params=pltpu.CompilerParams(
            collective_id=1, has_side_effects=True, vmem_limit_bytes=VMEM_LIMIT),
        name="reduce_gradient",
    )(x1, x2, y1)


def local(dims, hidden, queries, cotangent, point_start, point_mid, point_end, curve_time):
    t_value = curve_time[0]
    blended = (
        (1.0 - t_value) ** 2 * point_start.astype(jnp.float32)
        + 2.0 * t_value * (1.0 - t_value) * point_mid.astype(jnp.float32)
        + t_value**2 * point_end.astype(jnp.float32)
    ).astype(jnp.bfloat16)
    rows, cols = point_mid.shape
    kv_rows, x2 = gather_project(dims, blended, hidden)
    context, kv_grad = attend(kv_rows, queries, cotangent)
    gradient = reduce_gradient(dims, hidden, x2, kv_grad, rows, cols)
    return (context, gradient * (2.0 * t_value * (1.0 - t_value)))


def solution(mesh):
    dp, fsdp = mesh.shape["dp"], mesh.shape["fsdp"]
    dims = (dp // 2, 2, fsdp // 2)
    return jax.shard_map(
        functools.partial(local, dims),
        mesh=mesh,
        in_specs=(
            P(("dp", "fsdp"), None),
            P(("dp", "fsdp"), None),
            P(("dp", "fsdp"), None),
            P("fsdp", "dp"),
            P("fsdp", "dp"),
            P("fsdp", "dp"),
            P(),
        ),
        out_specs=(P(("dp", "fsdp"), None), P("fsdp", "dp")),
        check_vma=False,
    )
```

```python
import functools
import math

import jax
import jax.numpy as jnp
from jax import lax
from jax.experimental import pallas as pl
from jax.experimental.pallas import tpu as pltpu
from jax.sharding import PartitionSpec as P

KVH = 4
HD = 128
BQ = 128
MESH = pl.DeviceIdType.MESH
VMEM_LIMIT = 60 * 1024 * 1024


def rope_tables(seq_len, head_dim):
    positions = jnp.arange(seq_len, dtype=jnp.float32)[:, None]
    halves_index = jnp.arange(head_dim // 2, dtype=jnp.float32)[None, :]
    inverse = jnp.exp(-(2.0 * halves_index / head_dim) * math.log(500000.0))
    angles = positions * inverse
    cosine = jnp.concatenate([jnp.cos(angles), jnp.cos(angles)], axis=1)
    sine_t = jnp.concatenate([jnp.sin(angles), jnp.sin(angles)], axis=1)
    return (cosine, sine_t)


def rotate(x):
    half = x.shape[-1] // 2
    return jnp.concatenate([-x[..., half:], x[..., :half]], axis=-1)


def rotate_back(x):
    half = x.shape[-1] // 2
    return jnp.concatenate([x[..., half:], -x[..., :half]], axis=-1)


NN = (((1,), (0,)), ((), ()))
NT = (((1,), (1,)), ((), ()))
TN = (((0,), (0,)), ((), ()))


def mm(x, y, dims=NN):
    return lax.dot_general(x, y, dims, preferred_element_type=jnp.float32)


def attend_kernel(k_ref, v_ref, q_ref, g_ref, cos_ref, sin_ref, ctx_ref, grad_ref, kg, vg):
    seq = k_ref.shape[0]
    group = q_ref.shape[1] // HD
    scale = 1.0 / math.sqrt(HD)
    to_base2 = scale * math.log2(math.e)
    raw = k_ref[...].astype(jnp.float32)
    cosine, sine_t = cos_ref[...], sin_ref[...]
    keys = (raw * cosine + rotate(raw) * sine_t).astype(jnp.bfloat16)
    values = v_ref[...]
    values_t = values.astype(jnp.float32).T.astype(jnp.bfloat16)
    kg[...] = jnp.zeros_like(kg)
    vg[...] = jnp.zeros_like(vg)
    for start in range(0, seq, BQ):
        nk = start + BQ
        rows = slice(start, nk)
        qs = jnp.concatenate([q_ref[rows, g * HD:(g + 1) * HD] for g in range(group)], axis=0)
        gs = jnp.concatenate([g_ref[rows, g * HD:(g + 1) * HD] for g in range(group)], axis=0)
        s = mm(keys[:nk], qs, NT)
        key_at = lax.broadcasted_iota(jnp.int32, (BQ, group * BQ), 0)
        query_at = lax.broadcasted_iota(jnp.int32, (BQ, group * BQ), 1) % BQ
        last = jnp.where(key_at <= query_at, s[start:], -1e30)
        s = last if start == 0 else jnp.concatenate([s[:start], last], axis=0)
        top = jnp.max(s, axis=0, keepdims=True)
        w = jnp.exp2((s - top) * to_base2)
        p = w * (1.0 / jnp.sum(w, axis=0, keepdims=True))
        p_low = p.astype(jnp.bfloat16)
        ctx_t = mm(values_t[:, :nk], p_low)
        dp = mm(values[:nk], gs, NT)
        vg[:nk] += mm(p_low, gs)
        delta = jnp.sum(dp * p, axis=0, keepdims=True)
        ds = (p * ((dp - delta) * scale)).astype(jnp.bfloat16)
        kg[:nk] += mm(ds, qs)
        ctx = ctx_t.T.astype(jnp.bfloat16)
        for g in range(group):
            ctx_ref[rows, g * HD:(g + 1) * HD] = ctx[g * BQ:(g + 1) * BQ]
    rot = kg[...]
    grad_ref[0] = (rot * cosine + rotate_back(rot * sine_t)).astype(jnp.bfloat16)
    grad_ref[1] = vg[...].astype(jnp.bfloat16)


def attend(kv_rows, queries, cotangent):
    seq = kv_rows.shape[0]
    heads = kv_rows.shape[1] // (2 * HD)
    width = queries.shape[1] // heads
    cosine, sine_t = rope_tables(seq, HD)
    return pl.pallas_call(
        attend_kernel,
        grid=(heads,),
        out_shape=(
            jax.ShapeDtypeStruct(queries.shape, jnp.bfloat16),
            jax.ShapeDtypeStruct((2, seq, heads * HD), jnp.bfloat16),
        ),
        in_specs=[
            pl.BlockSpec((seq, HD), lambda j: (0, j)),
            pl.BlockSpec((seq, HD), lambda j: (0, j + heads)),
            pl.BlockSpec((seq, width), lambda j: (0, j)),
            pl.BlockSpec((seq, width), lambda j: (0, j)),
            pl.BlockSpec((seq, HD), lambda j: (0, 0)),
            pl.BlockSpec((seq, HD), lambda j: (0, 0)),
        ],
        out_specs=(
            pl.BlockSpec((seq, width), lambda j: (0, j)),
            pl.BlockSpec((2, seq, HD), lambda j: (0, 0, j)),
        ),
        scratch_shapes=[pltpu.VMEM((seq, HD), jnp.float32), pltpu.VMEM((seq, HD), jnp.float32)],
        compiler_params=pltpu.CompilerParams(vmem_limit_bytes=VMEM_LIMIT),
        name="attend",
    )(kv_rows, kv_rows, queries, cotangent, cosine, sine_t)


ORDER = ((1, 0), (0, 1))


def place(dims):
    dp, fs = lax.axis_index("dp"), lax.axis_index("fsdp")
    return (dp // dims[1], dp % dims[1], fs // 2), fs % 2


def target(dims, at, core, axis=None, offset=0):
    at = list(at)
    if axis is not None:
        at[axis] = (at[axis] + offset) % dims[axis]
    return (at[0] * dims[1] + at[1], at[2] * 2 + core)


def greet(peers):
    barrier = pltpu.get_barrier_semaphore()
    for peer in peers:
        pl.semaphore_signal(barrier, inc=1, device_id=peer, device_id_type=MESH)
    pl.semaphore_wait(barrier, len(peers))


def send(src, dst, send_sem, recv_sem, peer):
    return pltpu.make_async_remote_copy(
        src_ref=src, dst_ref=dst, send_sem=send_sem, recv_sem=recv_sem,
        device_id=peer, device_id_type=MESH)


def all_peers(dims, at, core):
    peers = [target(dims, at, core, axis, k) for axis in range(3) for k in range(1, dims[axis])]
    return peers + [target(dims, at, 1 - core)]


def gather_kernel(dims, block_ref, hidden_ref, kv_ref, x2_ref, full, acc, load_sem, x_send, x_recv,
                  recv, z_send, s2, s3, c_send):
    at, core = place(dims)
    depth = dims[2]
    rows, cols = block_ref.shape
    half = rows // 2
    other = target(dims, at, 1 - core)

    def piece(c, h, zz, pos):
        return full.at[c, zz, pos[0], pos[1], pl.ds(h * half, half)]

    def cell(h, zz, pos):
        return recv.at[core, h, zz, pos[0], pos[1]]

    def moved(axis, k):
        pos = [at[0], at[1]]
        pos[axis] = (pos[axis] + k) % dims[axis]
        return pos

    def push(h, zz, pos, send_sem, peer):
        ref = piece(core, h, zz, pos)
        return send(ref, ref, send_sem, cell(h, zz, pos), peer)

    def to_z(h, zz, side):
        return push(h, zz, at[:2], z_send.at[h, side, zz],
                    target(dims, at, core, 2, (1, dims[2] - 1)[side]))

    def sides(act):
        pl.when(at[2] < depth - 1)(lambda: act(0))
        pl.when(at[2] > 0)(lambda: act(1))

    def near(k, act):
        below, above = at[2] - k, at[2] + k
        pl.when(below >= 0)(lambda: act(below, 0))
        pl.when(above < depth)(lambda: act(above, 1))

    def to_second(h, zz, k):
        d2 = ORDER[1 - h][0]
        return push(h, zz, at[:2], s2[h].at[k - 1, zz], target(dims, at, core, d2, k))

    def to_third(h, zz, pos, k):
        d2, d3 = ORDER[1 - h]
        return push(h, zz, pos, s3[h].at[k - 1, zz, pos[d2]], target(dims, at, core, d3, k))

    def to_core(h, zz, pos):
        ref = piece(core, h, zz, pos)
        return send(ref, ref, c_send.at[h, zz, pos[0], pos[1]], cell(h, zz, pos), other)

    def swap(zz):
        src = pl.multiple_of((2 * zz + 1 - core) * rows, rows)
        dst = pl.multiple_of(zz * rows, rows)
        return send(hidden_ref.at[:, pl.ds(src, rows)], x2_ref.at[:, pl.ds(dst, rows)],
                    x_send.at[zz], x_recv.at[zz], other)

    def arrived(c, h, zz, pos):
        ref = piece(c, h, zz, pos)
        send(ref, ref, c_send.at[h, zz, pos[0], pos[1]], recv.at[c, h, zz, pos[0], pos[1]],
             other).wait_recv()

    def relay_first(h, zz):
        d2, d3 = ORDER[1 - h]
        for k in range(1, dims[d2]):
            to_second(h, zz, k).start()
        for k in range(1, dims[d3]):
            to_third(h, zz, at[:2], k).start()
        to_core(h, zz, at[:2]).start()

    def relay_second(zz):
        for h in range(2):
            d2, d3 = ORDER[1 - h]
            for k2 in range(1, dims[d2]):
                pos = moved(d2, k2)
                arrived(core, h, zz, pos)
                for k in range(1, dims[d3]):
                    to_third(h, zz, pos, k).start()
                to_core(h, zz, pos).start()

    def product(c, zz, first):
        x = hidden_ref[:, pl.ds(pl.multiple_of((2 * zz + c) * rows, rows), rows)]
        for dp in range(dims[0] * dims[1]):
            w = full[c, zz, dp // dims[1], dp % dims[1]]
            got = mm(x, w)
            if first:
                acc[:, dp * cols:(dp + 1) * cols] = got
            else:
                acc[:, dp * cols:(dp + 1) * cols] += got

    def relay_third(zz):
        for h in range(2):
            d2, d3 = ORDER[1 - h]
            for k3 in range(1, dims[d3]):
                for k2 in range(dims[d2]):
                    pos = moved(d3, k3)
                    pos[d2] = (at[d2] + k2) % dims[d2]
                    arrived(core, h, zz, pos)
                    to_core(h, zz, pos).start()

    def from_core(zz):
        for h in range(2):
            for i in range(dims[0]):
                for j in range(dims[1]):
                    arrived(1 - core, h, zz, (i, j))

    loads = [pltpu.make_async_copy(block_ref.at[pl.ds(h * half, half)], piece(core, h, at[2], at[:2]),
                                   load_sem.at[h]) for h in range(2)]
    for load in loads:
        load.start()
    greet(all_peers(dims, at, core))
    for load in loads:
        load.wait()
    def start_z(zz, side):
        for h in range(2):
            to_z(h, zz, side).start()

    sides(lambda side: start_z(at[2], side))
    for h in range(2):
        relay_first(h, at[2])

    def take_z(zz, side):
        for h in range(2):
            arrived(core, h, zz, at[:2])
        more = at[2] < depth - 1 if side == 0 else at[2] > 0
        pl.when(more)(lambda: start_z(zz, side))
        for h in range(2):
            relay_first(h, zz)

    near(1, take_z)
    relay_second(at[2])

    @pl.loop(2, depth)
    def _(k):
        near(k, take_z)
        near(k - 1, lambda zz, side: relay_second(zz))

    near(depth - 1, lambda zz, side: relay_second(zz))

    @pl.loop(0, depth)
    def _(zz):
        swap(zz).start()

    relay_third(at[2])
    product(core, at[2], True)

    def finish_core(zz):
        from_core(zz)
        product(1 - core, zz, False)

    def third_near(zz, side):
        relay_third(zz)
        product(core, zz, False)

    near(1, third_near)
    finish_core(at[2])

    @pl.loop(2, depth)
    def _(k):
        near(k, third_near)
        near(k - 1, lambda zz, side: finish_core(zz))

    near(depth - 1, lambda zz, side: finish_core(zz))
    kv_ref[...] = acc[...].astype(jnp.bfloat16)

    @pl.loop(0, depth)
    def _(zz):
        for h in range(2):
            pl.when((zz <= at[2]) & (at[2] < depth - 1))(lambda: to_z(h, zz, 0).wait_send())
            pl.when((zz >= at[2]) & (at[2] > 0))(lambda: to_z(h, zz, 1).wait_send())

    @pl.loop(0, depth)
    def _(zz):
        swap(zz).wait()
        for h in range(2):
            d2, d3 = ORDER[1 - h]
            for k in range(1, dims[d2]):
                to_second(h, zz, k).wait_send()
            for k in range(1, dims[d3]):
                for k2 in range(dims[d2]):
                    pos = moved(d2, k2)
                    to_third(h, zz, pos, k).wait_send()
            for i in range(dims[0]):
                for j in range(dims[1]):
                    to_core(h, zz, (i, j)).wait_send()


def gather_project(dims, blended, hidden):
    rows, cols = blended.shape
    seq = hidden.shape[0]
    a, b, z = dims
    width = a * b * cols
    sem = pltpu.SemaphoreType.DMA

    def body(*refs):
        gather_kernel(dims, *refs[:10], refs[10], (refs[11], refs[12]), (refs[13], refs[14]), refs[15])

    def sems(h):
        d2, d3 = ORDER[1 - h]
        return dims[d2], dims[d3]

    vmem = pl.BlockSpec(memory_space=pltpu.VMEM)
    return pl.pallas_call(
        body,
        out_shape=(
            jax.ShapeDtypeStruct((seq, width), jnp.bfloat16),
            jax.ShapeDtypeStruct((seq, z * rows), jnp.bfloat16),
        ),
        in_specs=[pl.BlockSpec(memory_space=pl.ANY), vmem],
        out_specs=(vmem, pl.BlockSpec(memory_space=pl.ANY)),
        scratch_shapes=[
            pltpu.VMEM((2, z, a, b, rows, cols), jnp.bfloat16),
            pltpu.VMEM((seq, width), jnp.float32),
            sem((2,)), sem((z,)), sem((z,)),
            sem((2, 2, z, a, b)),
            sem((2, 2, z)),
            *[sem((sems(h)[0] - 1, z)) for h in range(2)],
            *[sem((sems(h)[1] - 1, z, sems(h)[0])) for h in range(2)],
            sem((2, z, a, b)),
        ],
        compiler_params=pltpu.CompilerParams(
            collective_id=2, has_side_effects=True, vmem_limit_bytes=VMEM_LIMIT),
        name="gather_project",
    )(blended, hidden)


def reduce_kernel(dims, x1_ref, x2_ref, y1_ref, out_ref, y2_ref, swap_send, swap_recv, *scratch):
    halves = [scratch[:11], scratch[11:]]
    at, core = place(dims)
    depth = dims[2]
    rows, cols = out_ref.shape
    half = rows // 2
    parts = y1_ref.shape[0]
    width = y1_ref.shape[2]
    other = target(dims, at, 1 - core)
    greet(all_peers(dims, at, core))
    swap = send(y1_ref, y2_ref, swap_send, swap_recv, other)
    swap.start()
    swap.wait()

    def first_copy(h, k1, zz):
        d1 = ORDER[h][0]
        part, r1, s1, q1 = halves[h][0], halves[h][1], halves[h][5], halves[h][6]
        v1 = (at[d1] + k1) % dims[d1]
        return send(part.at[zz, v1], r1.at[k1 - 1, zz], s1.at[k1 - 1, zz], q1.at[k1 - 1, zz],
                    target(dims, at, core, d1, k1))

    def second_copy(h, k2, zz):
        d2 = ORDER[h][1]
        sum2, r2, s2, q2 = halves[h][2], halves[h][3], halves[h][7], halves[h][8]
        return send(sum2.at[k2 - 1, zz], r2.at[k2 - 1, zz], s2.at[k2 - 1, zz], q2.at[k2 - 1, zz],
                    target(dims, at, core, d2, k2))

    def third_copy(h, k):
        r3, s3, q3 = halves[h][4], halves[h][9], halves[h][10]
        part = halves[h][0]
        zz = (at[2] + k) % depth
        d1, d2 = ORDER[h]
        return send(part.at[zz, at[d1], at[d2]], r3.at[k - 1], s3.at[k - 1], q3.at[k - 1],
                    target(dims, at, core, 2, k))

    def compute(step):
        zz = (at[2] + step) % depth
        x1 = x1_ref[:, pl.ds(pl.multiple_of((2 * zz + core) * rows, rows), rows)]
        x2 = x2_ref[:, pl.ds(pl.multiple_of(zz * rows, rows), rows)]
        for part in range(parts):
            r = (mm(x1, y1_ref[part], TN) + mm(x2, y2_ref[part], TN)).astype(jnp.bfloat16)
            for i in range(width // cols):
                dp = part * (width // cols) + i
                where = (dp // dims[1], dp % dims[1])
                for h in range(2):
                    d1, d2 = ORDER[h]
                    halves[h][0][zz, where[d1], where[d2]] = (
                        r[h * half:(h + 1) * half, i * cols:(i + 1) * cols])
        for h in range(2):
            for k1 in range(1, dims[ORDER[h][0]]):
                first_copy(h, k1, zz).start()

    def keep1(h, zz, v2):
        d1, d2 = ORDER[h]
        part, r1 = halves[h][0], halves[h][1]
        total = part[zz, at[d1], v2].astype(jnp.float32)
        for k1 in range(1, dims[d1]):
            total += r1[k1 - 1, zz, v2].astype(jnp.float32)
        return total

    def second(step):
        zz = (at[2] + step) % depth
        for h in range(2):
            d1, d2 = ORDER[h]
            for k1 in range(1, dims[d1]):
                first_copy(h, k1, zz).wait_recv()
            for k2 in range(1, dims[d2]):
                v2 = (at[d2] + k2) % dims[d2]
                halves[h][2][k2 - 1, zz] = keep1(h, zz, v2).astype(jnp.bfloat16)
                second_copy(h, k2, zz).start()

    def keep2(h, zz):
        d1, d2 = ORDER[h]
        total = keep1(h, zz, at[d2])
        for k2 in range(1, dims[d2]):
            second_copy(h, k2, zz).wait_recv()
        for k2 in range(1, dims[d2]):
            total += halves[h][3][k2 - 1, zz].astype(jnp.float32)
        return total

    def third(step):
        zz = (at[2] + step) % depth
        for h in range(2):
            d1, d2 = ORDER[h]
            halves[h][0][zz, at[d1], at[d2]] = keep2(h, zz).astype(jnp.bfloat16)
            third_copy(h, step).start()

    @pl.loop(1, 3)
    def _(step):
        compute(step)

    second(1)

    @pl.loop(3, depth + 1)
    def _(step):
        compute(step)
        second(step - 1)
        third(step - 2)

    second(depth)
    third(depth - 1)

    for h in range(2):
        total = keep2(h, at[2])
        for k in range(1, depth):
            third_copy(h, k).wait_recv()
            total += halves[h][4][k - 1].astype(jnp.float32)
        out_ref[h * half:(h + 1) * half] = total

    @pl.loop(0, depth)
    def _(zz):
        for h in range(2):
            for k1 in range(1, dims[ORDER[h][0]]):
                first_copy(h, k1, zz).wait_send()
            for k2 in range(1, dims[ORDER[h][1]]):
                second_copy(h, k2, zz).wait_send()

    @pl.loop(1, depth)
    def _(k):
        for h in range(2):
            third_copy(h, k).wait_send()


def reduce_gradient(dims, x1, x2, y1, rows, cols):
    half = rows // 2
    scratch = [pltpu.VMEM(y1.shape, y1.dtype), pltpu.SemaphoreType.DMA, pltpu.SemaphoreType.DMA]
    for h in range(2):
        n1, n2 = dims[ORDER[h][0]], dims[ORDER[h][1]]
        z = dims[2]
        scratch += [
            pltpu.VMEM((z, n1, n2, half, cols), jnp.bfloat16),
            pltpu.VMEM((n1 - 1, z, n2, half, cols), jnp.bfloat16),
            pltpu.VMEM((n2 - 1, z, half, cols), jnp.bfloat16),
            pltpu.VMEM((n2 - 1, z, half, cols), jnp.bfloat16),
            pltpu.VMEM((z - 1, half, cols), jnp.bfloat16),
            pltpu.SemaphoreType.DMA((n1 - 1, z)), pltpu.SemaphoreType.DMA((n1 - 1, z)),
            pltpu.SemaphoreType.DMA((n2 - 1, z)), pltpu.SemaphoreType.DMA((n2 - 1, z)),
            pltpu.SemaphoreType.DMA((z - 1,)), pltpu.SemaphoreType.DMA((z - 1,)),
        ]
    vmem = pl.BlockSpec(memory_space=pltpu.VMEM)
    return pl.pallas_call(
        functools.partial(reduce_kernel, dims),
        out_shape=jax.ShapeDtypeStruct((rows, cols), jnp.float32),
        in_specs=[vmem] * 3,
        out_specs=vmem,
        scratch_shapes=scratch,
        compiler_params=pltpu.CompilerParams(
            collective_id=1, has_side_effects=True, vmem_limit_bytes=VMEM_LIMIT),
        name="reduce_gradient",
    )(x1, x2, y1)


def local(dims, hidden, queries, cotangent, point_start, point_mid, point_end, curve_time):
    t_value = curve_time[0]
    blended = (
        (1.0 - t_value) ** 2 * point_start.astype(jnp.float32)
        + 2.0 * t_value * (1.0 - t_value) * point_mid.astype(jnp.float32)
        + t_value**2 * point_end.astype(jnp.float32)
    ).astype(jnp.bfloat16)
    rows, cols = point_mid.shape
    kv_rows, x2 = gather_project(dims, blended, hidden)
    context, kv_grad = attend(kv_rows, queries, cotangent)
    gradient = reduce_gradient(dims, hidden, x2, kv_grad, rows, cols)
    return (context, gradient * (2.0 * t_value * (1.0 - t_value)))


def solution(mesh):
    dp, fsdp = mesh.shape["dp"], mesh.shape["fsdp"]
    dims = (dp // 2, 2, fsdp // 2)
    return jax.shard_map(
        functools.partial(local, dims),
        mesh=mesh,
        in_specs=(
            P(("dp", "fsdp"), None),
            P(("dp", "fsdp"), None),
            P(("dp", "fsdp"), None),
            P("fsdp", "dp"),
            P("fsdp", "dp"),
            P("fsdp", "dp"),
            P(),
        ),
        out_specs=(P(("dp", "fsdp"), None), P("fsdp", "dp")),
        check_vma=False,
    )
```

```python
import functools
import math

import jax
import jax.numpy as jnp
from jax import lax
from jax.experimental import pallas as pl
from jax.experimental.pallas import tpu as pltpu
from jax.sharding import PartitionSpec as P

KVH = 4
HD = 128
BQ = 128
MESH = pl.DeviceIdType.MESH
VMEM_LIMIT = 60 * 1024 * 1024


def rope_tables(seq_len, head_dim):
    shape = (seq_len, head_dim)
    positions = lax.broadcasted_iota(jnp.int32, shape, 0).astype(jnp.float32)
    column = lax.broadcasted_iota(jnp.int32, shape, 1)
    halves_index = jnp.where(column < head_dim // 2, column, column - head_dim // 2).astype(jnp.float32)
    inverse = jnp.exp(-(2.0 * halves_index / head_dim) * math.log(500000.0))
    angles = positions * inverse
    cosine, sine_t = jnp.cos(angles), jnp.sin(angles)
    return (cosine, sine_t)


def rotate(x):
    half = x.shape[-1] // 2
    return jnp.concatenate([-x[..., half:], x[..., :half]], axis=-1)


def rotate_back(x):
    half = x.shape[-1] // 2
    return jnp.concatenate([x[..., half:], -x[..., :half]], axis=-1)


NN = (((1,), (0,)), ((), ()))
NT = (((1,), (1,)), ((), ()))
TN = (((0,), (0,)), ((), ()))


def mm(x, y, dims=NN):
    return lax.dot_general(x, y, dims, preferred_element_type=jnp.float32)


def attend_kernel(k_ref, v_ref, q_ref, g_ref, cos_ref, sin_ref, ctx_ref, grad_ref, kg, vg):
    seq = k_ref.shape[0]
    group = q_ref.shape[1] // HD
    scale = 1.0 / math.sqrt(HD)
    to_base2 = scale * math.log2(math.e)
    raw = k_ref[...].astype(jnp.float32)
    cosine, sine_t = cos_ref[...], sin_ref[...]
    keys = (raw * cosine + rotate(raw) * sine_t).astype(jnp.bfloat16)
    values = v_ref[...]
    values_t = values.astype(jnp.float32).T.astype(jnp.bfloat16)
    kg[...] = jnp.zeros_like(kg)
    vg[...] = jnp.zeros_like(vg)
    for start in range(0, seq, BQ):
        nk = start + BQ
        rows = slice(start, nk)
        qs = jnp.concatenate([q_ref[rows, g * HD:(g + 1) * HD] for g in range(group)], axis=0)
        gs = jnp.concatenate([g_ref[rows, g * HD:(g + 1) * HD] for g in range(group)], axis=0)
        s = mm(keys[:nk], qs, NT)
        key_at = lax.broadcasted_iota(jnp.int32, (BQ, group * BQ), 0)
        query_at = lax.broadcasted_iota(jnp.int32, (BQ, group * BQ), 1) % BQ
        last = jnp.where(key_at <= query_at, s[start:], -1e30)
        s = last if start == 0 else jnp.concatenate([s[:start], last], axis=0)
        top = jnp.max(s, axis=0, keepdims=True)
        w = jnp.exp2((s - top) * to_base2)
        p = w * (1.0 / jnp.sum(w, axis=0, keepdims=True))
        p_low = p.astype(jnp.bfloat16)
        ctx_t = mm(values_t[:, :nk], p_low)
        dp = mm(values[:nk], gs, NT)
        vg[:nk] += mm(p_low, gs)
        delta = jnp.sum(dp * p, axis=0, keepdims=True)
        ds = (p * ((dp - delta) * scale)).astype(jnp.bfloat16)
        kg[:nk] += mm(ds, qs)
        ctx = ctx_t.T.astype(jnp.bfloat16)
        for g in range(group):
            ctx_ref[rows, g * HD:(g + 1) * HD] = ctx[g * BQ:(g + 1) * BQ]
    rot = kg[...]
    grad_ref[0] = (rot * cosine + rotate_back(rot * sine_t)).astype(jnp.bfloat16)
    grad_ref[1] = vg[...].astype(jnp.bfloat16)


def attend(kv_rows, queries, cotangent, cosine, sine_t):
    seq = kv_rows.shape[0]
    heads = kv_rows.shape[1] // (2 * HD)
    width = queries.shape[1] // heads
    return pl.pallas_call(
        attend_kernel,
        grid=(heads,),
        out_shape=(
            jax.ShapeDtypeStruct(queries.shape, jnp.bfloat16),
            jax.ShapeDtypeStruct((2, seq, heads * HD), jnp.bfloat16),
        ),
        in_specs=[
            pl.BlockSpec((seq, HD), lambda j: (0, j)),
            pl.BlockSpec((seq, HD), lambda j: (0, j + heads)),
            pl.BlockSpec((seq, width), lambda j: (0, j)),
            pl.BlockSpec((seq, width), lambda j: (0, j)),
            pl.BlockSpec((seq, HD), lambda j: (0, 0)),
            pl.BlockSpec((seq, HD), lambda j: (0, 0)),
        ],
        out_specs=(
            pl.BlockSpec((seq, width), lambda j: (0, j)),
            pl.BlockSpec((2, seq, HD), lambda j: (0, 0, j)),
        ),
        scratch_shapes=[pltpu.VMEM((seq, HD), jnp.float32), pltpu.VMEM((seq, HD), jnp.float32)],
        compiler_params=pltpu.CompilerParams(vmem_limit_bytes=VMEM_LIMIT),
        name="attend",
    )(kv_rows, kv_rows, queries, cotangent, cosine, sine_t)


ORDER = ((1, 0), (0, 1))


def place(dims):
    dp, fs = lax.axis_index("dp"), lax.axis_index("fsdp")
    return (dp // dims[1], dp % dims[1], fs // 2), fs % 2


def target(dims, at, core, axis=None, offset=0):
    at = list(at)
    if axis is not None:
        at[axis] = (at[axis] + offset) % dims[axis]
    return (at[0] * dims[1] + at[1], at[2] * 2 + core)


def greet(peers):
    barrier = pltpu.get_barrier_semaphore()
    for peer in peers:
        pl.semaphore_signal(barrier, inc=1, device_id=peer, device_id_type=MESH)
    pl.semaphore_wait(barrier, len(peers))


def send(src, dst, send_sem, recv_sem, peer):
    return pltpu.make_async_remote_copy(
        src_ref=src, dst_ref=dst, send_sem=send_sem, recv_sem=recv_sem,
        device_id=peer, device_id_type=MESH)


def all_peers(dims, at, core):
    peers = [target(dims, at, core, axis, k) for axis in range(3) for k in range(1, dims[axis])]
    return peers + [target(dims, at, 1 - core)]


def gather_kernel(dims, block_ref, hidden_ref, kv_ref, x2_ref, cos_ref, sin_ref, full, acc, hid, load_sem, x_send, x_recv,
                  recv, z_send, s2, s3, c_send):
    at, core = place(dims)
    depth = dims[2]
    rows, cols = block_ref.shape
    half = rows // 2
    other = target(dims, at, 1 - core)

    def piece(c, h, zz, pos):
        return full.at[c, zz, pos[0], pos[1], pl.ds(h * half, half)]

    def cell(h, zz, pos):
        return recv.at[core, h, zz, pos[0], pos[1]]

    def moved(axis, k):
        pos = [at[0], at[1]]
        pos[axis] = (pos[axis] + k) % dims[axis]
        return pos

    def push(h, zz, pos, send_sem, peer):
        ref = piece(core, h, zz, pos)
        return send(ref, ref, send_sem, cell(h, zz, pos), peer)

    def to_z(h, zz, side):
        return push(h, zz, at[:2], z_send.at[h, side, zz],
                    target(dims, at, core, 2, (1, dims[2] - 1)[side]))

    def sides(act):
        pl.when(at[2] < depth - 1)(lambda: act(0))
        pl.when(at[2] > 0)(lambda: act(1))

    def near(k, act):
        below, above = at[2] - k, at[2] + k
        pl.when(below >= 0)(lambda: act(below, 0))
        pl.when(above < depth)(lambda: act(above, 1))

    def to_second(h, zz, k):
        d2 = ORDER[1 - h][0]
        return push(h, zz, at[:2], s2[h].at[k - 1, zz], target(dims, at, core, d2, k))

    def to_third(h, zz, pos, k):
        d2, d3 = ORDER[1 - h]
        return push(h, zz, pos, s3[h].at[k - 1, zz, pos[d2]], target(dims, at, core, d3, k))

    def to_core(h, zz, pos):
        ref = piece(core, h, zz, pos)
        return send(ref, ref, c_send.at[h, zz, pos[0], pos[1]], cell(h, zz, pos), other)

    def swap(zz):
        src = pl.multiple_of((2 * zz + 1 - core) * rows, rows)
        dst = pl.multiple_of(zz * rows, rows)
        return send(hidden_ref.at[:, pl.ds(src, rows)], x2_ref.at[:, pl.ds(dst, rows)],
                    x_send.at[zz], x_recv.at[zz], other)

    def arrived(c, h, zz, pos):
        ref = piece(c, h, zz, pos)
        send(ref, ref, c_send.at[h, zz, pos[0], pos[1]], recv.at[c, h, zz, pos[0], pos[1]],
             other).wait_recv()

    def relay_first(h, zz):
        d2, d3 = ORDER[1 - h]
        for k in range(1, dims[d2]):
            to_second(h, zz, k).start()
        for k in range(1, dims[d3]):
            to_third(h, zz, at[:2], k).start()
        to_core(h, zz, at[:2]).start()

    def relay_second(zz):
        for h in range(2):
            d2, d3 = ORDER[1 - h]
            for k2 in range(1, dims[d2]):
                pos = moved(d2, k2)
                arrived(core, h, zz, pos)
                for k in range(1, dims[d3]):
                    to_third(h, zz, pos, k).start()
                to_core(h, zz, pos).start()

    def product(c, zz, first):
        x = hid[:, pl.ds(pl.multiple_of((2 * zz + c) * rows, rows), rows)]
        for dp in range(dims[0] * dims[1]):
            w = full[c, zz, dp // dims[1], dp % dims[1]]
            got = mm(x, w)
            if first:
                acc[:, dp * cols:(dp + 1) * cols] = got
            else:
                acc[:, dp * cols:(dp + 1) * cols] += got

    def relay_third(zz):
        for h in range(2):
            d2, d3 = ORDER[1 - h]
            for k3 in range(1, dims[d3]):
                for k2 in range(dims[d2]):
                    pos = moved(d3, k3)
                    pos[d2] = (at[d2] + k2) % dims[d2]
                    arrived(core, h, zz, pos)
                    to_core(h, zz, pos).start()

    def from_core(zz):
        for h in range(2):
            for i in range(dims[0]):
                for j in range(dims[1]):
                    arrived(1 - core, h, zz, (i, j))

    loads = [pltpu.make_async_copy(block_ref.at[pl.ds(h * half, half)], piece(core, h, at[2], at[:2]),
                                   load_sem.at[h]) for h in range(2)]
    for load in loads:
        load.start()
    whole = pltpu.make_async_copy(hidden_ref, hid, load_sem.at[2])
    whole.start()
    greet(all_peers(dims, at, core))
    for load in loads:
        load.wait()
    def start_z(zz, side):
        for h in range(2):
            to_z(h, zz, side).start()

    sides(lambda side: start_z(at[2], side))
    for h in range(2):
        relay_first(h, at[2])

    @pl.loop(0, depth)
    def _(zz):
        swap(zz).start()

    cosine, sine_t = rope_tables(*cos_ref.shape)
    cos_ref[...] = cosine
    sin_ref[...] = sine_t

    def take_z(zz, side):
        for h in range(2):
            arrived(core, h, zz, at[:2])
        more = at[2] < depth - 1 if side == 0 else at[2] > 0
        pl.when(more)(lambda: start_z(zz, side))
        for h in range(2):
            relay_first(h, zz)

    near(1, take_z)
    relay_second(at[2])

    @pl.loop(2, depth)
    def _(k):
        near(k, take_z)
        near(k - 1, lambda zz, side: relay_second(zz))

    near(depth - 1, lambda zz, side: relay_second(zz))

    whole.wait()
    relay_third(at[2])
    product(core, at[2], True)

    def finish_core(zz):
        from_core(zz)
        product(1 - core, zz, False)

    def third_near(zz, side):
        relay_third(zz)
        product(core, zz, False)

    near(1, third_near)
    finish_core(at[2])

    @pl.loop(2, depth)
    def _(k):
        near(k, third_near)
        near(k - 1, lambda zz, side: finish_core(zz))

    near(depth - 1, lambda zz, side: finish_core(zz))
    kv_ref[...] = acc[...].astype(jnp.bfloat16)

    @pl.loop(0, depth)
    def _(zz):
        for h in range(2):
            pl.when((zz <= at[2]) & (at[2] < depth - 1))(lambda: to_z(h, zz, 0).wait_send())
            pl.when((zz >= at[2]) & (at[2] > 0))(lambda: to_z(h, zz, 1).wait_send())

    @pl.loop(0, depth)
    def _(zz):
        swap(zz).wait()
        for h in range(2):
            d2, d3 = ORDER[1 - h]
            for k in range(1, dims[d2]):
                to_second(h, zz, k).wait_send()
            for k in range(1, dims[d3]):
                for k2 in range(dims[d2]):
                    pos = moved(d2, k2)
                    to_third(h, zz, pos, k).wait_send()
            for i in range(dims[0]):
                for j in range(dims[1]):
                    to_core(h, zz, (i, j)).wait_send()


def gather_project(dims, blended, hidden):
    rows, cols = blended.shape
    seq = hidden.shape[0]
    a, b, z = dims
    width = a * b * cols
    sem = pltpu.SemaphoreType.DMA

    def body(*refs):
        gather_kernel(dims, *refs[:14], (refs[14], refs[15]), (refs[16], refs[17]), refs[18])

    def sems(h):
        d2, d3 = ORDER[1 - h]
        return dims[d2], dims[d3]

    vmem = pl.BlockSpec(memory_space=pltpu.VMEM)
    return pl.pallas_call(
        body,
        out_shape=(
            jax.ShapeDtypeStruct((seq, width), jnp.bfloat16),
            jax.ShapeDtypeStruct((seq, z * rows), jnp.bfloat16),
            jax.ShapeDtypeStruct((seq, HD), jnp.float32),
            jax.ShapeDtypeStruct((seq, HD), jnp.float32),
        ),
        in_specs=[pl.BlockSpec(memory_space=pl.ANY)] * 2,
        out_specs=(vmem, pl.BlockSpec(memory_space=pl.ANY), vmem, vmem),
        scratch_shapes=[
            pltpu.VMEM((2, z, a, b, rows, cols), jnp.bfloat16),
            pltpu.VMEM((seq, width), jnp.float32),
            pltpu.VMEM(hidden.shape, hidden.dtype),
            sem((3,)), sem((z,)), sem((z,)),
            sem((2, 2, z, a, b)),
            sem((2, 2, z)),
            *[sem((sems(h)[0] - 1, z)) for h in range(2)],
            *[sem((sems(h)[1] - 1, z, sems(h)[0])) for h in range(2)],
            sem((2, z, a, b)),
        ],
        compiler_params=pltpu.CompilerParams(
            collective_id=2, has_side_effects=True, vmem_limit_bytes=VMEM_LIMIT),
        name="gather_project",
    )(blended, hidden)


def reduce_kernel(dims, h_ref, x2_ref, y1_ref, out_ref, y2_ref, swap_send, swap_recv, xs, xsem, early,
                  *scratch):
    halves = [scratch[:11], scratch[11:]]
    at, core = place(dims)
    depth = dims[2]
    rows, cols = out_ref.shape
    half = rows // 2
    parts = y1_ref.shape[0]
    width = y1_ref.shape[2]
    other = target(dims, at, 1 - core)
    def loads(zz):
        own = pl.multiple_of((2 * zz + core) * rows, rows)
        theirs = pl.multiple_of(zz * rows, rows)
        return (pltpu.make_async_copy(h_ref.at[:, pl.ds(own, rows)], xs.at[0, zz], xsem.at[0, zz]),
                pltpu.make_async_copy(x2_ref.at[:, pl.ds(theirs, rows)], xs.at[1, zz], xsem.at[1, zz]))

    @pl.loop(1, depth + 1)
    def _(step):
        for load in loads((at[2] + step) % depth):
            load.start()

    greet(all_peers(dims, at, core))
    swap = send(y1_ref, y2_ref, swap_send, swap_recv, other)
    swap.start()

    def first_copy(h, k1, zz):
        d1 = ORDER[h][0]
        part, r1, s1, q1 = halves[h][0], halves[h][1], halves[h][5], halves[h][6]
        v1 = (at[d1] + k1) % dims[d1]
        return send(part.at[zz, v1], r1.at[k1 - 1, zz], s1.at[k1 - 1, zz], q1.at[k1 - 1, zz],
                    target(dims, at, core, d1, k1))

    def second_copy(h, k2, zz):
        d2 = ORDER[h][1]
        sum2, r2, s2, q2 = halves[h][2], halves[h][3], halves[h][7], halves[h][8]
        return send(sum2.at[k2 - 1, zz], r2.at[k2 - 1, zz], s2.at[k2 - 1, zz], q2.at[k2 - 1, zz],
                    target(dims, at, core, d2, k2))

    def third_copy(h, k):
        r3, s3, q3 = halves[h][4], halves[h][9], halves[h][10]
        part = halves[h][0]
        zz = (at[2] + k) % depth
        d1, d2 = ORDER[h]
        return send(part.at[zz, at[d1], at[d2]], r3.at[k - 1], s3.at[k - 1], q3.at[k - 1],
                    target(dims, at, core, 2, k))

    def compute(step, peeled=False):
        zz = (at[2] + step) % depth
        own, theirs = loads(zz)
        if not peeled:
            own.wait()
        theirs.wait()
        for part in range(parts):
            first = early[part] if peeled else mm(xs[0, zz], y1_ref[part], TN)
            r = (first + mm(xs[1, zz], y2_ref[part], TN)).astype(jnp.bfloat16)
            for i in range(width // cols):
                dp = part * (width // cols) + i
                where = (dp // dims[1], dp % dims[1])
                for h in range(2):
                    d1, d2 = ORDER[h]
                    halves[h][0][zz, where[d1], where[d2]] = (
                        r[h * half:(h + 1) * half, i * cols:(i + 1) * cols])
        for h in range(2):
            for k1 in range(1, dims[ORDER[h][0]]):
                first_copy(h, k1, zz).start()

    def keep1(h, zz, v2):
        d1, d2 = ORDER[h]
        part, r1 = halves[h][0], halves[h][1]
        total = part[zz, at[d1], v2].astype(jnp.float32)
        for k1 in range(1, dims[d1]):
            total += r1[k1 - 1, zz, v2].astype(jnp.float32)
        return total

    def second(step):
        zz = (at[2] + step) % depth
        for h in range(2):
            d1, d2 = ORDER[h]
            for k1 in range(1, dims[d1]):
                first_copy(h, k1, zz).wait_recv()
            for k2 in range(1, dims[d2]):
                v2 = (at[d2] + k2) % dims[d2]
                halves[h][2][k2 - 1, zz] = keep1(h, zz, v2).astype(jnp.bfloat16)
                second_copy(h, k2, zz).start()

    def keep2(h, zz):
        d1, d2 = ORDER[h]
        total = keep1(h, zz, at[d2])
        for k2 in range(1, dims[d2]):
            second_copy(h, k2, zz).wait_recv()
        for k2 in range(1, dims[d2]):
            total += halves[h][3][k2 - 1, zz].astype(jnp.float32)
        return total

    def third(step):
        zz = (at[2] + step) % depth
        for h in range(2):
            d1, d2 = ORDER[h]
            halves[h][0][zz, at[d1], at[d2]] = keep2(h, zz).astype(jnp.bfloat16)
            third_copy(h, step).start()

    start = (at[2] + 1) % depth
    loads(start)[0].wait()
    for part in range(parts):
        early[part] = mm(xs[0, start], y1_ref[part], TN)
    swap.wait()
    compute(1, True)
    compute(2)
    second(1)

    @pl.loop(3, depth + 1)
    def _(step):
        compute(step)
        second(step - 1)
        third(step - 2)

    second(depth)
    third(depth - 1)

    for h in range(2):
        total = keep2(h, at[2])
        for k in range(1, depth):
            third_copy(h, k).wait_recv()
            total += halves[h][4][k - 1].astype(jnp.float32)
        out_ref[h * half:(h + 1) * half] = total

    @pl.loop(0, depth)
    def _(zz):
        for h in range(2):
            for k1 in range(1, dims[ORDER[h][0]]):
                first_copy(h, k1, zz).wait_send()
            for k2 in range(1, dims[ORDER[h][1]]):
                second_copy(h, k2, zz).wait_send()

    @pl.loop(1, depth)
    def _(k):
        for h in range(2):
            third_copy(h, k).wait_send()


def reduce_gradient(dims, x1, x2, y1, rows, cols):
    half = rows // 2
    scratch = [
        pltpu.VMEM(y1.shape, y1.dtype), pltpu.SemaphoreType.DMA, pltpu.SemaphoreType.DMA,
        pltpu.VMEM((2, dims[2], y1.shape[1], rows), jnp.bfloat16),
        pltpu.SemaphoreType.DMA((2, dims[2])),
        pltpu.VMEM((y1.shape[0], rows, y1.shape[2]), jnp.float32),
    ]
    for h in range(2):
        n1, n2 = dims[ORDER[h][0]], dims[ORDER[h][1]]
        z = dims[2]
        scratch += [
            pltpu.VMEM((z, n1, n2, half, cols), jnp.bfloat16),
            pltpu.VMEM((n1 - 1, z, n2, half, cols), jnp.bfloat16),
            pltpu.VMEM((n2 - 1, z, half, cols), jnp.bfloat16),
            pltpu.VMEM((n2 - 1, z, half, cols), jnp.bfloat16),
            pltpu.VMEM((z - 1, half, cols), jnp.bfloat16),
            pltpu.SemaphoreType.DMA((n1 - 1, z)), pltpu.SemaphoreType.DMA((n1 - 1, z)),
            pltpu.SemaphoreType.DMA((n2 - 1, z)), pltpu.SemaphoreType.DMA((n2 - 1, z)),
            pltpu.SemaphoreType.DMA((z - 1,)), pltpu.SemaphoreType.DMA((z - 1,)),
        ]
    vmem = pl.BlockSpec(memory_space=pltpu.VMEM)
    return pl.pallas_call(
        functools.partial(reduce_kernel, dims),
        out_shape=jax.ShapeDtypeStruct((rows, cols), jnp.float32),
        in_specs=[pl.BlockSpec(memory_space=pl.ANY)] * 2 + [vmem],
        out_specs=vmem,
        scratch_shapes=scratch,
        compiler_params=pltpu.CompilerParams(
            collective_id=1, has_side_effects=True, vmem_limit_bytes=VMEM_LIMIT),
        name="reduce_gradient",
    )(x1, x2, y1)


def local(dims, hidden, queries, cotangent, point_start, point_mid, point_end, curve_time):
    t_value = curve_time[0]
    blended = (
        (1.0 - t_value) ** 2 * point_start.astype(jnp.float32)
        + 2.0 * t_value * (1.0 - t_value) * point_mid.astype(jnp.float32)
        + t_value**2 * point_end.astype(jnp.float32)
    ).astype(jnp.bfloat16)
    rows, cols = point_mid.shape
    kv_rows, x2, cosine, sine_t = gather_project(dims, blended, hidden)
    context, kv_grad = attend(kv_rows, queries, cotangent, cosine, sine_t)
    gradient = reduce_gradient(dims, hidden, x2, kv_grad, rows, cols)
    return (context, gradient * (2.0 * t_value * (1.0 - t_value)))


def solution(mesh):
    dp, fsdp = mesh.shape["dp"], mesh.shape["fsdp"]
    dims = (dp // 2, 2, fsdp // 2)
    return jax.shard_map(
        functools.partial(local, dims),
        mesh=mesh,
        in_specs=(
            P(("dp", "fsdp"), None),
            P(("dp", "fsdp"), None),
            P(("dp", "fsdp"), None),
            P("fsdp", "dp"),
            P("fsdp", "dp"),
            P("fsdp", "dp"),
            P(),
        ),
        out_specs=(P(("dp", "fsdp"), None), P("fsdp", "dp")),
        check_vma=False,
    )
```

```python
import functools
import math

import jax
import jax.numpy as jnp
from jax import lax
from jax.experimental import pallas as pl
from jax.experimental.pallas import tpu as pltpu
from jax.sharding import PartitionSpec as P

KVH = 4
HD = 128
BQ = 256
MESH = pl.DeviceIdType.MESH
VMEM_LIMIT = 60 * 1024 * 1024


def rope_tables(seq_len, head_dim):
    shape = (seq_len, head_dim)
    positions = lax.broadcasted_iota(jnp.int32, shape, 0).astype(jnp.float32)
    column = lax.broadcasted_iota(jnp.int32, shape, 1)
    halves_index = jnp.where(column < head_dim // 2, column, column - head_dim // 2).astype(jnp.float32)
    inverse = jnp.exp(-(2.0 * halves_index / head_dim) * math.log(500000.0))
    angles = positions * inverse
    cosine, sine_t = jnp.cos(angles), jnp.sin(angles)
    return (cosine, sine_t)


def rotate(x):
    half = x.shape[-1] // 2
    return jnp.concatenate([-x[..., half:], x[..., :half]], axis=-1)


def rotate_back(x):
    half = x.shape[-1] // 2
    return jnp.concatenate([x[..., half:], -x[..., :half]], axis=-1)


NN = (((1,), (0,)), ((), ()))
NT = (((1,), (1,)), ((), ()))
TN = (((0,), (0,)), ((), ()))


def mm(x, y, dims=NN):
    return lax.dot_general(x, y, dims, preferred_element_type=jnp.float32)


def attend_kernel(k_ref, v_ref, q_ref, g_ref, cos_ref, sin_ref, ctx_ref, grad_ref, kg, vg):
    seq = k_ref.shape[0]
    group = q_ref.shape[1] // HD
    scale = 1.0 / math.sqrt(HD)
    to_base2 = scale * math.log2(math.e)
    raw = k_ref[...].astype(jnp.float32)
    cosine, sine_t = cos_ref[...], sin_ref[...]
    keys = (raw * cosine + rotate(raw) * sine_t).astype(jnp.bfloat16)
    values = v_ref[...]
    values_t = values.astype(jnp.float32).T.astype(jnp.bfloat16)
    kg[...] = jnp.zeros_like(kg)
    vg[...] = jnp.zeros_like(vg)
    for start in range(0, seq, BQ):
        nk = start + BQ
        rows = slice(start, nk)
        qs = jnp.concatenate([q_ref[rows, g * HD:(g + 1) * HD] for g in range(group)], axis=0)
        gs = jnp.concatenate([g_ref[rows, g * HD:(g + 1) * HD] for g in range(group)], axis=0)
        s = mm(keys[:nk], qs, NT)
        key_at = lax.broadcasted_iota(jnp.int32, (BQ, group * BQ), 0)
        query_at = lax.broadcasted_iota(jnp.int32, (BQ, group * BQ), 1) % BQ
        last = jnp.where(key_at <= query_at, s[start:], -1e30)
        s = last if start == 0 else jnp.concatenate([s[:start], last], axis=0)
        top = jnp.max(s, axis=0, keepdims=True)
        w = jnp.exp2((s - top) * to_base2)
        p = w * (1.0 / jnp.sum(w, axis=0, keepdims=True))
        p_low = p.astype(jnp.bfloat16)
        ctx_t = mm(values_t[:, :nk], p_low)
        dp = mm(values[:nk], gs, NT)
        vg[:nk] += mm(p_low, gs)
        delta = jnp.sum(dp * p, axis=0, keepdims=True)
        ds = (p * ((dp - delta) * scale)).astype(jnp.bfloat16)
        kg[:nk] += mm(ds, qs)
        ctx = ctx_t.T.astype(jnp.bfloat16)
        for g in range(group):
            ctx_ref[rows, g * HD:(g + 1) * HD] = ctx[g * BQ:(g + 1) * BQ]
    rot = kg[...]
    grad_ref[0] = (rot * cosine + rotate_back(rot * sine_t)).astype(jnp.bfloat16)
    grad_ref[1] = vg[...].astype(jnp.bfloat16)


def attend(kv_rows, queries, cotangent, cosine, sine_t):
    seq = kv_rows.shape[0]
    heads = kv_rows.shape[1] // (2 * HD)
    width = queries.shape[1] // heads
    return pl.pallas_call(
        attend_kernel,
        grid=(heads,),
        out_shape=(
            jax.ShapeDtypeStruct(queries.shape, jnp.bfloat16),
            jax.ShapeDtypeStruct((2, seq, heads * HD), jnp.bfloat16),
        ),
        in_specs=[
            pl.BlockSpec((seq, HD), lambda j: (0, j)),
            pl.BlockSpec((seq, HD), lambda j: (0, j + heads)),
            pl.BlockSpec((seq, width), lambda j: (0, j)),
            pl.BlockSpec((seq, width), lambda j: (0, j)),
            pl.BlockSpec((seq, HD), lambda j: (0, 0)),
            pl.BlockSpec((seq, HD), lambda j: (0, 0)),
        ],
        out_specs=(
            pl.BlockSpec((seq, width), lambda j: (0, j)),
            pl.BlockSpec((2, seq, HD), lambda j: (0, 0, j)),
        ),
        scratch_shapes=[pltpu.VMEM((seq, HD), jnp.float32), pltpu.VMEM((seq, HD), jnp.float32)],
        compiler_params=pltpu.CompilerParams(vmem_limit_bytes=VMEM_LIMIT),
        name="attend",
    )(kv_rows, kv_rows, queries, cotangent, cosine, sine_t)


ORDER = ((1, 0), (0, 1))


def place(dims):
    dp, fs = lax.axis_index("dp"), lax.axis_index("fsdp")
    return (dp // dims[1], dp % dims[1], fs // 2), fs % 2


def target(dims, at, core, axis=None, offset=0):
    at = list(at)
    if axis is not None:
        at[axis] = (at[axis] + offset) % dims[axis]
    return (at[0] * dims[1] + at[1], at[2] * 2 + core)


def greet(peers):
    barrier = pltpu.get_barrier_semaphore()
    for peer in peers:
        pl.semaphore_signal(barrier, inc=1, device_id=peer, device_id_type=MESH)
    pl.semaphore_wait(barrier, len(peers))


def send(src, dst, send_sem, recv_sem, peer):
    return pltpu.make_async_remote_copy(
        src_ref=src, dst_ref=dst, send_sem=send_sem, recv_sem=recv_sem,
        device_id=peer, device_id_type=MESH)


def all_peers(dims, at, core):
    peers = [target(dims, at, core, axis, k) for axis in range(3) for k in range(1, dims[axis])]
    return peers + [target(dims, at, 1 - core)]


def gather_kernel(dims, block_ref, hidden_ref, kv_ref, x2_ref, cos_ref, sin_ref, full, acc, hid, load_sem, x_send, x_recv,
                  recv, z_send, s2, s3, c_send):
    at, core = place(dims)
    depth = dims[2]
    rows, cols = block_ref.shape
    half = rows // 2
    other = target(dims, at, 1 - core)

    def piece(c, h, zz, pos):
        return full.at[c, zz, pos[0], pos[1], pl.ds(h * half, half)]

    def cell(h, zz, pos):
        return recv.at[core, h, zz, pos[0], pos[1]]

    def moved(axis, k):
        pos = [at[0], at[1]]
        pos[axis] = (pos[axis] + k) % dims[axis]
        return pos

    def push(h, zz, pos, send_sem, peer):
        ref = piece(core, h, zz, pos)
        return send(ref, ref, send_sem, cell(h, zz, pos), peer)

    def to_z(h, zz, side):
        return push(h, zz, at[:2], z_send.at[h, side, zz],
                    target(dims, at, core, 2, (1, dims[2] - 1)[side]))

    def sides(act):
        pl.when(at[2] < depth - 1)(lambda: act(0))
        pl.when(at[2] > 0)(lambda: act(1))

    def near(k, act):
        below, above = at[2] - k, at[2] + k
        pl.when(below >= 0)(lambda: act(below, 0))
        pl.when(above < depth)(lambda: act(above, 1))

    def to_second(h, zz, k):
        d2 = ORDER[1 - h][0]
        return push(h, zz, at[:2], s2[h].at[k - 1, zz], target(dims, at, core, d2, k))

    def to_third(h, zz, pos, k):
        d2, d3 = ORDER[1 - h]
        return push(h, zz, pos, s3[h].at[k - 1, zz, pos[d2]], target(dims, at, core, d3, k))

    def to_core(h, zz, pos):
        ref = piece(core, h, zz, pos)
        return send(ref, ref, c_send.at[h, zz, pos[0], pos[1]], cell(h, zz, pos), other)

    def swap(zz):
        src = pl.multiple_of((2 * zz + 1 - core) * rows, rows)
        dst = pl.multiple_of(zz * rows, rows)
        return send(hidden_ref.at[:, pl.ds(src, rows)], x2_ref.at[:, pl.ds(dst, rows)],
                    x_send.at[zz], x_recv.at[zz], other)

    def arrived(c, h, zz, pos):
        ref = piece(c, h, zz, pos)
        send(ref, ref, c_send.at[h, zz, pos[0], pos[1]], recv.at[c, h, zz, pos[0], pos[1]],
             other).wait_recv()

    def relay_first(h, zz):
        d2, d3 = ORDER[1 - h]
        for k in range(1, dims[d2]):
            to_second(h, zz, k).start()
        for k in range(1, dims[d3]):
            to_third(h, zz, at[:2], k).start()
        to_core(h, zz, at[:2]).start()

    def relay_second(zz):
        for h in range(2):
            d2, d3 = ORDER[1 - h]
            for k2 in range(1, dims[d2]):
                pos = moved(d2, k2)
                arrived(core, h, zz, pos)
                for k in range(1, dims[d3]):
                    to_third(h, zz, pos, k).start()
                to_core(h, zz, pos).start()

    def product(c, zz, first):
        x = hid[:, pl.ds(pl.multiple_of((2 * zz + c) * rows, rows), rows)]
        for dp in range(dims[0] * dims[1]):
            w = full[c, zz, dp // dims[1], dp % dims[1]]
            got = mm(x, w)
            if first:
                acc[:, dp * cols:(dp + 1) * cols] = got
            else:
                acc[:, dp * cols:(dp + 1) * cols] += got

    def relay_third(zz):
        for h in range(2):
            d2, d3 = ORDER[1 - h]
            for k3 in range(1, dims[d3]):
                for k2 in range(dims[d2]):
                    pos = moved(d3, k3)
                    pos[d2] = (at[d2] + k2) % dims[d2]
                    arrived(core, h, zz, pos)
                    to_core(h, zz, pos).start()

    def from_core(zz):
        for h in range(2):
            for i in range(dims[0]):
                for j in range(dims[1]):
                    arrived(1 - core, h, zz, (i, j))

    loads = [pltpu.make_async_copy(block_ref.at[pl.ds(h * half, half)], piece(core, h, at[2], at[:2]),
                                   load_sem.at[h]) for h in range(2)]
    for load in loads:
        load.start()
    whole = pltpu.make_async_copy(hidden_ref, hid, load_sem.at[2])
    whole.start()
    greet(all_peers(dims, at, core))
    for load in loads:
        load.wait()
    def start_z(zz, side):
        for h in range(2):
            to_z(h, zz, side).start()

    sides(lambda side: start_z(at[2], side))
    for h in range(2):
        relay_first(h, at[2])

    @pl.loop(0, depth)
    def _(zz):
        swap(zz).start()

    cosine, sine_t = rope_tables(*cos_ref.shape)
    cos_ref[...] = cosine
    sin_ref[...] = sine_t

    def take_z(zz, side):
        for h in range(2):
            arrived(core, h, zz, at[:2])
        more = at[2] < depth - 1 if side == 0 else at[2] > 0
        pl.when(more)(lambda: start_z(zz, side))
        for h in range(2):
            relay_first(h, zz)

    near(1, take_z)
    relay_second(at[2])

    @pl.loop(2, depth)
    def _(k):
        near(k, take_z)
        near(k - 1, lambda zz, side: relay_second(zz))

    near(depth - 1, lambda zz, side: relay_second(zz))

    whole.wait()
    relay_third(at[2])
    product(core, at[2], True)

    def finish_core(zz):
        from_core(zz)
        product(1 - core, zz, False)

    def third_near(zz, side):
        relay_third(zz)
        product(core, zz, False)

    near(1, third_near)
    finish_core(at[2])

    @pl.loop(2, depth)
    def _(k):
        near(k, third_near)
        near(k - 1, lambda zz, side: finish_core(zz))

    near(depth - 1, lambda zz, side: finish_core(zz))
    kv_ref[...] = acc[...].astype(jnp.bfloat16)

    @pl.loop(0, depth)
    def _(zz):
        for h in range(2):
            pl.when((zz <= at[2]) & (at[2] < depth - 1))(lambda: to_z(h, zz, 0).wait_send())
            pl.when((zz >= at[2]) & (at[2] > 0))(lambda: to_z(h, zz, 1).wait_send())

    @pl.loop(0, depth)
    def _(zz):
        swap(zz).wait()
        for h in range(2):
            d2, d3 = ORDER[1 - h]
            for k in range(1, dims[d2]):
                to_second(h, zz, k).wait_send()
            for k in range(1, dims[d3]):
                for k2 in range(dims[d2]):
                    pos = moved(d2, k2)
                    to_third(h, zz, pos, k).wait_send()
            for i in range(dims[0]):
                for j in range(dims[1]):
                    to_core(h, zz, (i, j)).wait_send()


def gather_project(dims, blended, hidden):
    rows, cols = blended.shape
    seq = hidden.shape[0]
    a, b, z = dims
    width = a * b * cols
    sem = pltpu.SemaphoreType.DMA

    def body(*refs):
        gather_kernel(dims, *refs[:14], (refs[14], refs[15]), (refs[16], refs[17]), refs[18])

    def sems(h):
        d2, d3 = ORDER[1 - h]
        return dims[d2], dims[d3]

    vmem = pl.BlockSpec(memory_space=pltpu.VMEM)
    return pl.pallas_call(
        body,
        out_shape=(
            jax.ShapeDtypeStruct((seq, width), jnp.bfloat16),
            jax.ShapeDtypeStruct((seq, z * rows), jnp.bfloat16),
            jax.ShapeDtypeStruct((seq, HD), jnp.float32),
            jax.ShapeDtypeStruct((seq, HD), jnp.float32),
        ),
        in_specs=[pl.BlockSpec(memory_space=pl.ANY)] * 2,
        out_specs=(vmem, pl.BlockSpec(memory_space=pl.ANY), vmem, vmem),
        scratch_shapes=[
            pltpu.VMEM((2, z, a, b, rows, cols), jnp.bfloat16),
            pltpu.VMEM((seq, width), jnp.float32),
            pltpu.VMEM(hidden.shape, hidden.dtype),
            sem((3,)), sem((z,)), sem((z,)),
            sem((2, 2, z, a, b)),
            sem((2, 2, z)),
            *[sem((sems(h)[0] - 1, z)) for h in range(2)],
            *[sem((sems(h)[1] - 1, z, sems(h)[0])) for h in range(2)],
            sem((2, z, a, b)),
        ],
        compiler_params=pltpu.CompilerParams(
            collective_id=2, has_side_effects=True, vmem_limit_bytes=VMEM_LIMIT),
        name="gather_project",
    )(blended, hidden)


def reduce_kernel(dims, h_ref, x2_ref, y1_ref, out_ref, y2_ref, swap_send, swap_recv, xs, xsem, early,
                  *scratch):
    halves = [scratch[:11], scratch[11:]]
    at, core = place(dims)
    depth = dims[2]
    rows, cols = out_ref.shape
    half = rows // 2
    parts = y1_ref.shape[0]
    width = y1_ref.shape[2]
    other = target(dims, at, 1 - core)
    def loads(zz):
        own = pl.multiple_of((2 * zz + core) * rows, rows)
        theirs = pl.multiple_of(zz * rows, rows)
        return (pltpu.make_async_copy(h_ref.at[:, pl.ds(own, rows)], xs.at[0, zz], xsem.at[0, zz]),
                pltpu.make_async_copy(x2_ref.at[:, pl.ds(theirs, rows)], xs.at[1, zz], xsem.at[1, zz]))

    @pl.loop(1, depth + 1)
    def _(step):
        for load in loads((at[2] + step) % depth):
            load.start()

    greet(all_peers(dims, at, core))
    swap = send(y1_ref, y2_ref, swap_send, swap_recv, other)
    swap.start()

    def first_copy(h, k1, zz):
        d1 = ORDER[h][0]
        part, r1, s1, q1 = halves[h][0], halves[h][1], halves[h][5], halves[h][6]
        v1 = (at[d1] + k1) % dims[d1]
        return send(part.at[zz, v1], r1.at[k1 - 1, zz], s1.at[k1 - 1, zz], q1.at[k1 - 1, zz],
                    target(dims, at, core, d1, k1))

    def second_copy(h, k2, zz):
        d2 = ORDER[h][1]
        sum2, r2, s2, q2 = halves[h][2], halves[h][3], halves[h][7], halves[h][8]
        return send(sum2.at[k2 - 1, zz], r2.at[k2 - 1, zz], s2.at[k2 - 1, zz], q2.at[k2 - 1, zz],
                    target(dims, at, core, d2, k2))

    def third_copy(h, k):
        r3, s3, q3 = halves[h][4], halves[h][9], halves[h][10]
        part = halves[h][0]
        zz = (at[2] + k) % depth
        d1, d2 = ORDER[h]
        return send(part.at[zz, at[d1], at[d2]], r3.at[k - 1], s3.at[k - 1], q3.at[k - 1],
                    target(dims, at, core, 2, k))

    def compute(step, peeled=False):
        zz = (at[2] + step) % depth
        own, theirs = loads(zz)
        if not peeled:
            own.wait()
        theirs.wait()
        for part in range(parts):
            first = early[part] if peeled else mm(xs[0, zz], y1_ref[part], TN)
            r = (first + mm(xs[1, zz], y2_ref[part], TN)).astype(jnp.bfloat16)
            for i in range(width // cols):
                dp = part * (width // cols) + i
                where = (dp // dims[1], dp % dims[1])
                for h in range(2):
                    d1, d2 = ORDER[h]
                    halves[h][0][zz, where[d1], where[d2]] = (
                        r[h * half:(h + 1) * half, i * cols:(i + 1) * cols])
        for h in range(2):
            for k1 in range(1, dims[ORDER[h][0]]):
                first_copy(h, k1, zz).start()

    def keep1(h, zz, v2):
        d1, d2 = ORDER[h]
        part, r1 = halves[h][0], halves[h][1]
        total = part[zz, at[d1], v2].astype(jnp.float32)
        for k1 in range(1, dims[d1]):
            total += r1[k1 - 1, zz, v2].astype(jnp.float32)
        return total

    def second(step):
        zz = (at[2] + step) % depth
        for h in range(2):
            d1, d2 = ORDER[h]
            for k1 in range(1, dims[d1]):
                first_copy(h, k1, zz).wait_recv()
            for k2 in range(1, dims[d2]):
                v2 = (at[d2] + k2) % dims[d2]
                halves[h][2][k2 - 1, zz] = keep1(h, zz, v2).astype(jnp.bfloat16)
                second_copy(h, k2, zz).start()

    def keep2(h, zz):
        d1, d2 = ORDER[h]
        total = keep1(h, zz, at[d2])
        for k2 in range(1, dims[d2]):
            second_copy(h, k2, zz).wait_recv()
        for k2 in range(1, dims[d2]):
            total += halves[h][3][k2 - 1, zz].astype(jnp.float32)
        return total

    def third(step):
        zz = (at[2] + step) % depth
        for h in range(2):
            d1, d2 = ORDER[h]
            halves[h][0][zz, at[d1], at[d2]] = keep2(h, zz).astype(jnp.bfloat16)
            third_copy(h, step).start()

    start = (at[2] + 1) % depth
    loads(start)[0].wait()
    for part in range(parts):
        early[part] = mm(xs[0, start], y1_ref[part], TN)
    swap.wait()
    compute(1, True)
    compute(2)
    second(1)

    @pl.loop(3, depth + 1)
    def _(step):
        compute(step)
        second(step - 1)
        third(step - 2)

    second(depth)
    third(depth - 1)

    for h in range(2):
        total = keep2(h, at[2])
        for k in range(1, depth):
            third_copy(h, k).wait_recv()
            total += halves[h][4][k - 1].astype(jnp.float32)
        out_ref[h * half:(h + 1) * half] = total

    @pl.loop(0, depth)
    def _(zz):
        for h in range(2):
            for k1 in range(1, dims[ORDER[h][0]]):
                first_copy(h, k1, zz).wait_send()
            for k2 in range(1, dims[ORDER[h][1]]):
                second_copy(h, k2, zz).wait_send()

    @pl.loop(1, depth)
    def _(k):
        for h in range(2):
            third_copy(h, k).wait_send()


def reduce_gradient(dims, x1, x2, y1, rows, cols):
    half = rows // 2
    scratch = [
        pltpu.VMEM(y1.shape, y1.dtype), pltpu.SemaphoreType.DMA, pltpu.SemaphoreType.DMA,
        pltpu.VMEM((2, dims[2], y1.shape[1], rows), jnp.bfloat16),
        pltpu.SemaphoreType.DMA((2, dims[2])),
        pltpu.VMEM((y1.shape[0], rows, y1.shape[2]), jnp.float32),
    ]
    for h in range(2):
        n1, n2 = dims[ORDER[h][0]], dims[ORDER[h][1]]
        z = dims[2]
        scratch += [
            pltpu.VMEM((z, n1, n2, half, cols), jnp.bfloat16),
            pltpu.VMEM((n1 - 1, z, n2, half, cols), jnp.bfloat16),
            pltpu.VMEM((n2 - 1, z, half, cols), jnp.bfloat16),
            pltpu.VMEM((n2 - 1, z, half, cols), jnp.bfloat16),
            pltpu.VMEM((z - 1, half, cols), jnp.bfloat16),
            pltpu.SemaphoreType.DMA((n1 - 1, z)), pltpu.SemaphoreType.DMA((n1 - 1, z)),
            pltpu.SemaphoreType.DMA((n2 - 1, z)), pltpu.SemaphoreType.DMA((n2 - 1, z)),
            pltpu.SemaphoreType.DMA((z - 1,)), pltpu.SemaphoreType.DMA((z - 1,)),
        ]
    vmem = pl.BlockSpec(memory_space=pltpu.VMEM)
    return pl.pallas_call(
        functools.partial(reduce_kernel, dims),
        out_shape=jax.ShapeDtypeStruct((rows, cols), jnp.float32),
        in_specs=[pl.BlockSpec(memory_space=pl.ANY)] * 2 + [vmem],
        out_specs=vmem,
        scratch_shapes=scratch,
        compiler_params=pltpu.CompilerParams(
            collective_id=1, has_side_effects=True, vmem_limit_bytes=VMEM_LIMIT),
        name="reduce_gradient",
    )(x1, x2, y1)


def local(dims, hidden, queries, cotangent, point_start, point_mid, point_end, curve_time):
    t_value = curve_time[0]
    blended = (
        (1.0 - t_value) ** 2 * point_start.astype(jnp.float32)
        + 2.0 * t_value * (1.0 - t_value) * point_mid.astype(jnp.float32)
        + t_value**2 * point_end.astype(jnp.float32)
    ).astype(jnp.bfloat16)
    rows, cols = point_mid.shape
    kv_rows, x2, cosine, sine_t = gather_project(dims, blended, hidden)
    context, kv_grad = attend(kv_rows, queries, cotangent, cosine, sine_t)
    gradient = reduce_gradient(dims, hidden, x2, kv_grad, rows, cols)
    return (context, gradient * (2.0 * t_value * (1.0 - t_value)))


def solution(mesh):
    dp, fsdp = mesh.shape["dp"], mesh.shape["fsdp"]
    dims = (dp // 2, 2, fsdp // 2)
    return jax.shard_map(
        functools.partial(local, dims),
        mesh=mesh,
        in_specs=(
            P(("dp", "fsdp"), None),
            P(("dp", "fsdp"), None),
            P(("dp", "fsdp"), None),
            P("fsdp", "dp"),
            P("fsdp", "dp"),
            P("fsdp", "dp"),
            P(),
        ),
        out_specs=(P(("dp", "fsdp"), None), P("fsdp", "dp")),
        check_vma=False,
    )
```
